32 devices in a mesh: grp: 2 (over y), ctx: 8 (over z, x), head: 2 (over core).
Axes of the slice: x: 2, y: 2, z: 4, core: 2. Of those that a mesh axis runs over, the one named last changes fastest.
Arguments:
- block_owner: int32 [32, 1], P('grp'), parts along dimension 0, may hold values from 0 to 7; in each aligned block of 16 rows (0 to 15, 16 to 31, ...) at most 6 rows name the same one
- block_slot: int32 [32], P('grp'), parts along dimension 0, may hold values from 0 to 1
- recv_keys: bfloat16 [4096, 1024], P(('grp', 'ctx'), 'head'), parts along dimension 0, may hold values from -4.5 to 4.5
- recv_values: bfloat16 [4096, 1024], P(('grp', 'ctx'), 'head'), parts along dimension 0, may hold values from -6 to 6
- sharer_values: bfloat16 [4096, 1024], P(('grp', 'ctx'), 'head'), parts along dimension 0, may hold values from -6 to 6
- queries: bfloat16 [16, 8192], P(('grp', 'ctx'), 'head'), parts along dimension 0, may hold values from -170 to 170
- new_keys: bfloat16 [16, 1024], P(('grp', 'ctx'), 'head'), parts along dimension 0, may hold values from -7 to 7
- new_values: bfloat16 [16, 1024], P(('grp', 'ctx'), 'head'), parts along dimension 0, may hold values from -6 to 6
- mixer_gate: bfloat16 [256, 2048], replicated, may hold values from -0.375 to 0.375
- mixer_up: bfloat16 [256, 2048], replicated, may hold values from -0.375 to 0.375
- mixer_down: bfloat16 [2048, 128], replicated, may hold values from -0.125 to 0.125
- gate_logit: float32 [8], P('head'), may hold values from -2 to 2
Outputs:
- merged_values: bfloat16 [4096, 1024], P(('grp', 'ctx'), 'head'), parts along dimension 0
- attended: bfloat16 [16, 8192], P(('grp', 'ctx'), 'head'), parts along dimension 0
The draws below stay inside these ranges and needn't reach their ends.
There are 2 independent parts, one for each index of `grp`. The reference program is written for one: setup_inputs(seed, part) draws one part's arguments, and reference() takes and returns one part's arrays. A program takes and returns all parts, laid end to end along the dimension named above; an argument that names none is the same for every part. Nothing has to cross between parts.
Inputs may be any that keep to these rules, and one draw needn't show every extreme that they name: `block_owner`: every owner is named by at least one sharer block and by at most 6; some owner by exactly 6.
All inputs are finite; a program needn't handle non-finite values.
Results may differ from the reference program's by a relative error of at most 0.0053.
Values may be sent and summed in bfloat16 or wider, within the bound.
No kernel may reach another device: no remote copies, remote signals or barrier semaphores. Data moves between devices by JAX's collectives and lax.ppermute only.
A program may use at most 64 MiB of HBM per device.

```python
import math
import jax
import jax.numpy as jnp
import numpy as np
from jax import lax

QH = 64
H_KV = 8
DH = 128
FH = 2048
BLK = 128
BLK_DEV = 2
SB = 16
CTX = 2048
QROWS = 8
G = 8
MOST = 6
N_CTX = 8


def drawn_keys(key):
    drawn = jax.random.normal(jax.random.fold_in(key, 11), (CTX, H_KV * DH), jnp.float32)
    return jnp.clip(drawn, -4.5, 4.5)


def draw_recv_keys(key, part):
    keys_now = drawn_keys(key)
    return keys_now.astype(jnp.bfloat16)


def draw_queries(key, part):
    drawn = jax.random.normal(jax.random.fold_in(key, 12), (QROWS, QH * DH), jnp.float32)
    drawn = 3.0 * jnp.clip(drawn, -4.0, 4.0)
    return drawn.astype(jnp.bfloat16)


def set_ends(entries, rng, least, largest):
    spot = [jax.random.randint(jax.random.fold_in(rng, axis), (), 0, length) for axis, length in enumerate(entries.shape)]
    main_axis = entries.shape.index(max(entries.shape))
    next_to = spot[:main_axis] + [(spot[main_axis] + 1) % entries.shape[main_axis]] + spot[main_axis + 1:]
    return entries.at[tuple(spot)].set(least).at[tuple(next_to)].set(largest)


def steps_of(rng, shape, cuts, least, high):
    gain = 1.0
    for dim, parts in cuts:
        draws = jax.random.uniform(jax.random.fold_in(jax.random.fold_in(rng, 6), dim), (parts,), jnp.float32, least / len(cuts), high / len(cuts))
        gain = gain * jnp.repeat(jnp.exp(draws), shape[dim] // parts).reshape((-1,) + (1,) * (len(shape) - 1 - dim))
    return gain


def routed_block(stream_key, own, number, rows, count, top, bound, lean):
    sequence = jax.random.permutation(stream_key, count)
    heavy_load, common = load_shares(count, rows * top, bound, lean, True), load_shares(count, rows * top, bound, lean, False)
    places = jnp.arange(count)

    def named(sizes, offset_by):
        used = int((sizes > 0).sum())
        fixed = max(1, used // 4)
        passed = fixed + (places - fixed + offset_by * (used - fixed)) % max(1, count - fixed)
        return jnp.zeros((count,), jnp.int32).at[sequence[jnp.where(places < fixed, places, passed)]].set(jnp.asarray(sizes, jnp.int32))

    sizes = jnp.where(number % 4 == 0, named(heavy_load, number // 4), named(common, number - number // 4 - 1))
    mixed = jax.random.permutation(jax.random.fold_in(own, 3), count)
    giver, taker = mixed[0:count // 2 * 2:2], mixed[1:count // 2 * 2:2]
    room = jnp.minimum(sizes[giver] - 1, bound - sizes[taker]) // 2
    room = jnp.where((giver == sequence[0]) | (taker == sequence[0]) | (sizes[taker] == 0), 0, jnp.maximum(room, 0))
    passed = jax.random.randint(jax.random.fold_in(own, 4), (count // 2,), 0, 1 << 20) % (room + 1)
    sizes = sizes.at[giver].add(-passed).at[taker].add(passed)
    members = jnp.searchsorted(jnp.cumsum(sizes), jnp.arange(rows * top), side="right").astype(jnp.int32)
    listing = members.reshape(top, rows).T
    listing = listing[jax.random.permutation(jax.random.fold_in(own, 1), rows)]
    offset_by = jax.random.randint(jax.random.fold_in(own, 2), (rows, 1), 0, top)
    return jnp.take_along_axis(listing, (jnp.arange(top)[None, :] + offset_by) % top, axis=1)


def load_shares(count, total, most, skew, full):
    weights = [(1 << 20) // math.isqrt(grade ** skew) + 1 for grade in range(1, count + 1)]
    largest = most if full else min(most, max(-(-total // count), total * weights[0] // sum(weights)))
    least = 1 if total - largest >= count - 1 else 0
    holding, rest = [largest] + [least] * (count - 1), total - largest - least * (count - 1)
    while rest > 0:
        movable = [i for i in range(1, count) if holding[i] < largest] or [i for i in range(1, count) if holding[i] < most]
        mass, remaining = sum([weights[i] for i in movable]), rest
        for i in movable:
            more = min(most - holding[i], max(1, remaining * weights[i] // mass), rest)
            holding[i] = holding[i] + more
            rest = rest - more
    return np.array(holding)


def gaussian(key, dims, deviation, most, cuts=(), kind=jnp.bfloat16):
    loudness = steps_of(key, dims, cuts, -0.22, 0.18) if cuts else 1.0
    entries = jax.random.normal(key, dims, jnp.float32) * deviation * loudness
    return jnp.minimum(jnp.maximum(entries, -most), most).astype(kind)


def setup_inputs(seed: int = 0, part: int = 0) -> dict:
    streams_of = jax.random.split(jax.random.key(seed), 13)
    part_splits = jax.random.split(jax.random.fold_in(streams_of[12], part), 13)
    block_owner_keys = jax.random.split(jax.random.fold_in(part_splits[0], 1), SB // SB)
    block_owner_turns = jax.random.permutation(jax.random.fold_in(part_splits[0], 3), SB // SB)
    block_owner = jax.vmap(lambda own, number: routed_block(jax.random.fold_in(part_splits[0], 2), own, number, SB, N_CTX, 1, MOST, 3))(block_owner_keys, block_owner_turns).reshape((SB, 1))
    block_slot = set_ends(jax.random.randint(part_splits[1], (SB,), 0, BLK_DEV), jax.random.fold_in(part_splits[1], 1), 0, BLK_DEV - 1).astype(jnp.int32)
    recv_keys = draw_recv_keys(jax.random.fold_in(jax.random.fold_in(streams_of[12], part), 71), part)
    recv_values = gaussian(part_splits[3], (CTX, H_KV * DH), 1.0, 6.0, ((0, 8), (1, 2)))
    sharer_values = gaussian(part_splits[4], (CTX, H_KV * DH), 1.0, 6.0, ((0, 8), (1, 2)))
    queries = draw_queries(jax.random.fold_in(jax.random.fold_in(streams_of[12], part), 71), part)
    new_keys = gaussian(part_splits[6], (QROWS, H_KV * DH), 1.6, 7.0, ((0, 8), (1, 2)))
    new_values = gaussian(part_splits[7], (QROWS, H_KV * DH), 1.0, 6.0, ((0, 8), (1, 2)))
    mixer_gate = gaussian(streams_of[8], (2 * DH, FH), (2 * DH) ** -0.5, 0.375)
    mixer_up = gaussian(streams_of[9], (2 * DH, FH), (2 * DH) ** -0.5, 0.375)
    mixer_down = gaussian(streams_of[10], (FH, DH), FH ** -0.5, 0.125)
    gate_logit = jnp.clip(jax.random.uniform(streams_of[11], (H_KV,), jnp.float32, -2.0, 2.0) * steps_of(streams_of[11], (H_KV,), ((0, 2),), -0.4, 0.0), -2.0, 2.0)
    return dict(block_owner=block_owner, block_slot=block_slot, recv_keys=recv_keys, recv_values=recv_values, sharer_values=sharer_values, queries=queries, new_keys=new_keys, new_values=new_values, mixer_gate=mixer_gate, mixer_up=mixer_up, mixer_down=mixer_down, gate_logit=gate_logit)


def mixer_block(value_block, aligned_block, mixer_gate, mixer_up, mixer_down, head_gates):
    row_count = value_block.shape[0] * value_block.shape[1]
    joined = jnp.concatenate([value_block, aligned_block], axis=2).reshape(row_count, 2 * value_block.shape[2])
    gate_pre = jnp.dot(joined, mixer_gate, preferred_element_type=jnp.float32)
    up_pre = jnp.dot(joined, mixer_up, preferred_element_type=jnp.float32)
    hidden = (jax.nn.silu(gate_pre) * up_pre).astype(jnp.bfloat16)
    update = jnp.dot(hidden, mixer_down, preferred_element_type=jnp.float32).reshape(value_block.shape)
    merged = value_block.astype(jnp.float32) + head_gates[None, :, None] * update
    return merged.astype(jnp.bfloat16)

def reference(block_owner, block_slot, recv_keys, recv_values, sharer_values, queries, new_keys, new_values, mixer_gate, mixer_up, mixer_down, gate_logit):
    blocks = CTX // BLK
    dest_block = (block_owner[:, 0] * BLK_DEV + block_slot).astype(jnp.int32)
    unit_weights = jnp.ones((blocks,), jnp.float32)
    block_count = jax.ops.segment_sum(unit_weights, dest_block, num_segments=blocks)
    flat_sharer = sharer_values.reshape(blocks, BLK * H_KV * DH).astype(jnp.float32)
    block_sums = jax.ops.segment_sum(flat_sharer, dest_block, num_segments=blocks)
    aligned = (block_sums / jnp.maximum(block_count, 1.0)[:, None]).astype(jnp.bfloat16)
    aligned = aligned.reshape(blocks, BLK, H_KV, DH)
    value_blocks = recv_values.reshape(blocks, BLK, H_KV, DH)
    head_gates = jax.nn.sigmoid(gate_logit)

    def blend_pair(block_pair):
        return mixer_block(block_pair[0], block_pair[1], mixer_gate, mixer_up, mixer_down, head_gates)
    merged_values = lax.map(blend_pair, (value_blocks, aligned)).reshape(CTX, H_KV * DH)
    score_scale = 1.0 / math.sqrt(DH)
    query_heads = queries.reshape(QROWS, H_KV, G, DH).transpose(1, 0, 2, 3)
    key_heads = recv_keys.reshape(CTX, H_KV, DH).transpose(1, 0, 2)
    value_heads = merged_values.reshape(CTX, H_KV, DH).transpose(1, 0, 2)
    new_key_heads = new_keys.reshape(QROWS, H_KV, DH).transpose(1, 0, 2)
    new_value_heads = new_values.reshape(QROWS, H_KV, DH).transpose(1, 0, 2)
    causal = jnp.arange(QROWS)[None, :] <= jnp.arange(QROWS)[:, None]

    def attend_head(head_items):
        query_one, key_one, value_one, new_key_one, new_value_one = head_items
        query_wide = query_one.astype(jnp.float32)
        scores = jnp.einsum('qgd,kd->qgk', query_wide, key_one.astype(jnp.float32)) * score_scale
        fresh = jnp.einsum('qgd,ud->qgu', query_wide, new_key_one.astype(jnp.float32)) * score_scale
        fresh = jnp.where(causal[:, None, :], fresh, -jnp.inf)
        row_top = jnp.maximum(lax.optimization_barrier(jnp.max(scores, axis=2)), lax.optimization_barrier(jnp.max(fresh, axis=2)))
        weights = jnp.exp(scores - row_top[:, :, None])
        fresh_weights = jnp.exp(fresh - row_top[:, :, None])
        denominator = lax.optimization_barrier(jnp.sum(weights, axis=2)) + lax.optimization_barrier(jnp.sum(fresh_weights, axis=2))
        rounded = lax.optimization_barrier(weights.astype(jnp.bfloat16))
        fresh_rounded = lax.optimization_barrier(fresh_weights.astype(jnp.bfloat16))
        numerator = jnp.einsum('qgk,kd->qgd', rounded.astype(jnp.float32), value_one.astype(jnp.float32))
        numerator = numerator + jnp.einsum('qgu,ud->qgd', fresh_rounded.astype(jnp.float32), new_value_one.astype(jnp.float32))
        return (numerator / denominator[:, :, None]).astype(jnp.bfloat16)
    per_head = lax.map(attend_head, (query_heads, key_heads, value_heads, new_key_heads, new_value_heads))
    attended = per_head.transpose(1, 0, 2, 3).reshape(QROWS, QH * DH)
    return (merged_values, attended)
```

```python
import functools
import math

import jax
import jax.numpy as jnp
from jax import lax
from jax.experimental import pallas as pl
from jax.experimental.pallas import tpu as pltpu
from jax.sharding import PartitionSpec as P

DH = 128
BLK = 128
G = 8
STAT = 8
NEG = -1e30
SMEM = pl.BlockSpec(memory_space=pltpu.SMEM)
VMEM = pl.BlockSpec(memory_space=pltpu.VMEM)


def exchange(x):
    return lax.all_to_all(x, "ctx", split_axis=0, concat_axis=0, tiled=True)


def query_tile(query_ref, scratch):
    for r in range(scratch.shape[0]):
        scratch[r : r + 1, :] = query_ref[0:1, r * DH : (r + 1) * DH].astype(jnp.float32)
    return scratch[...].astype(jnp.bfloat16)


def pack_kernel(sharer_ref, query_ref, out_ref, scratch, *, blocks, slice_len):
    devices = out_ref.shape[0]
    width = sharer_ref.shape[1]
    q = query_tile(query_ref, scratch)
    for d in range(devices):
        for k in range(blocks):
            start = k * BLK + d * slice_len
            out_ref[d, k * slice_len : (k + 1) * slice_len, :width] = sharer_ref[
                start : start + slice_len, :
            ]
        out_ref[d, :, width:] = q


def align_kernel(owner_ref, slot_ref, got_ref, out_ref, sums, counts, *, blocks, slice_len):
    devices = out_ref.shape[0]
    width = out_ref.shape[2]
    total = devices * blocks
    sums[...] = jnp.zeros(sums.shape, jnp.float32)
    for r in range(total):
        counts[r] = 0
    for b in range(total):
        dest = owner_ref[b] * blocks + slot_ref[b]
        s, k = divmod(b, blocks)
        sums[dest] += got_ref[s, k * slice_len : (k + 1) * slice_len, :width].astype(jnp.float32)
        counts[dest] = counts[dest] + 1
    for r in range(total):
        d, k = divmod(r, blocks)
        many = jnp.full((1, width), jnp.maximum(counts[r], 1), jnp.int32).astype(jnp.float32)
        out_ref[d, k * slice_len : (k + 1) * slice_len, :] = (sums[r] / many).astype(jnp.bfloat16)


def score_kernel(place_ref, got_ref, key_ref, new_key_ref, new_value_ref, weight_ref, part_ref, *, heads):
    rows = got_ref.shape[0]
    scale = 1.0 / math.sqrt(DH)
    q_all = got_ref[:, :, got_ref.shape[2] - DH :].astype(jnp.float32)
    row_of = lax.broadcasted_iota(jnp.int32, (rows * G, 1), 0) // G
    allowed = row_of >= place_ref[0]
    sub = lax.broadcasted_iota(jnp.int32, (1, G, DH), 1)
    lane = lax.broadcasted_iota(jnp.int32, (1, G, DH), 2)
    tops = jnp.zeros((rows, 1, DH), jnp.float32)
    dens = jnp.zeros((rows, 1, DH), jnp.float32)
    for j in range(heads):
        cols = slice(j * DH, (j + 1) * DH)
        q = q_all[:, j * G : (j + 1) * G, :].reshape(rows * G, DH)
        s = (
            lax.dot_general(
                q.astype(jnp.bfloat16),
                key_ref[:, cols],
                (((1,), (1,)), ((), ())),
                preferred_element_type=jnp.float32,
            )
            * scale
        )
        sf = jnp.sum(q * new_key_ref[0:1, cols].astype(jnp.float32), axis=1, keepdims=True) * scale
        top = jnp.maximum(
            jnp.max(s, axis=1, keepdims=True), jnp.where(allowed, sf, NEG)
        )
        w = jnp.exp(s - top)
        wf = jnp.where(allowed, jnp.exp(jnp.where(allowed, sf, top) - top), 0.0)
        den = jnp.sum(w, axis=1, keepdims=True) + wf
        weight_ref[j] = w.astype(jnp.bfloat16)
        fresh = wf.astype(jnp.bfloat16).astype(jnp.float32) * new_value_ref[0:1, cols].astype(
            jnp.float32
        )
        part_ref[:, j * G : (j + 1) * G, :] = fresh.reshape(rows, G, DH)
        here = lane == sub + j * G
        spread = lambda v: jnp.sum(
            jnp.where(here, jnp.broadcast_to(v, (rows * G, DH)).reshape(rows, G, DH), 0.0),
            axis=1,
            keepdims=True,
        )
        tops += spread(top)
        dens += spread(den)
    part_ref[:, heads * G :, :] = jnp.where(
        sub == 0, jnp.broadcast_to(tops, (rows, STAT, DH)), jnp.broadcast_to(dens, (rows, STAT, DH))
    )


def mixer_kernel(
    logit_ref, got_ref, value_ref, gate_ref, up_ref, down_ref, weight_ref, part_ref, merged_ref, out_ref,
    *, blocks, slice_len, chunk
):
    tokens, width = value_ref.shape
    heads = width // DH
    hidden = gate_ref.shape[1]
    rows = part_ref.shape[0]
    out_ref[:, heads * G :, :] = part_ref[:, heads * G :, :]
    for j in range(heads):
        cols = slice(j * DH, (j + 1) * DH)
        v = value_ref[:, cols]
        if slice_len:
            a = jnp.concatenate(
                [
                    got_ref[s, k * slice_len : (k + 1) * slice_len, cols]
                    for k in range(blocks)
                    for s in range(got_ref.shape[0])
                ],
                axis=0,
            )
        else:
            a = got_ref[:, cols]
        x = jnp.concatenate([v, a], axis=1)
        update = jnp.zeros((tokens, DH), jnp.float32)
        for c in range(0, hidden, chunk):
            g = jnp.dot(x, gate_ref[:, c : c + chunk], preferred_element_type=jnp.float32)
            u = jnp.dot(x, up_ref[:, c : c + chunk], preferred_element_type=jnp.float32)
            half = g * 0.5
            h = ((half + half * jnp.tanh(half)) * u).astype(jnp.bfloat16)
            update += jnp.dot(h, down_ref[c : c + chunk, :], preferred_element_type=jnp.float32)
        head_gate = jax.nn.sigmoid(jnp.full((1, DH), logit_ref[j], jnp.float32))
        merged = (v.astype(jnp.float32) + head_gate * update).astype(jnp.bfloat16)
        merged_ref[:, cols] = merged
        numer = jnp.dot(weight_ref[j], merged, preferred_element_type=jnp.float32)
        out_ref[:, j * G : (j + 1) * G, :] = part_ref[:, j * G : (j + 1) * G, :] + numer.reshape(
            rows, G, DH
        )


def combine_kernel(got_ref, out_ref, scratch, *, heads):
    n = heads * G
    tops = got_ref[:, n : n + 1, :]
    dens = got_ref[:, n + 1 : n + 2, :]
    factor = jnp.exp(tops - jnp.max(tops, axis=0, keepdims=True))
    factor = factor / jnp.sum(factor * dens, axis=0, keepdims=True)
    sub = lax.broadcasted_iota(jnp.int32, (1, n, DH), 1)
    lane = lax.broadcasted_iota(jnp.int32, (1, n, DH), 2)
    column = jnp.sum(jnp.where(lane == sub, factor, 0.0), axis=2, keepdims=True)
    scratch[...] = jnp.sum(column * got_ref[:, :n, :], axis=0)
    for r in range(n):
        out_ref[0:1, r * DH : (r + 1) * DH] = scratch[r : r + 1, :].astype(jnp.bfloat16)


def body(
    block_owner, block_slot, recv_keys, recv_values, sharer_values, queries, new_keys, new_values,
    mixer_gate, mixer_up, mixer_down, gate_logit,
):
    devices = lax.axis_size("ctx")
    place = lax.axis_index("ctx").astype(jnp.int32).reshape(1)
    tokens, width = recv_values.shape
    heads = width // DH
    blocks = tokens // BLK
    total = blocks * devices
    slice_len = BLK // devices
    owner = block_owner[:, 0]
    rows = devices
    tiled = slice_len % 16 == 0
    f32, bf16 = jnp.float32, jnp.bfloat16
    shape = jax.ShapeDtypeStruct

    if tiled:
        send = pl.pallas_call(
            functools.partial(pack_kernel, blocks=blocks, slice_len=slice_len),
            out_shape=shape((devices, blocks * slice_len, width + DH), bf16),
            scratch_shapes=[pltpu.VMEM((heads * G, DH), f32)],
            name="pack",
        )(sharer_values, queries)
        got = exchange(send)
        mean = pl.pallas_call(
            functools.partial(align_kernel, blocks=blocks, slice_len=slice_len),
            out_shape=shape((devices, blocks * slice_len, width), bf16),
            in_specs=[SMEM, SMEM, VMEM],
            scratch_shapes=[pltpu.VMEM((total, slice_len, width), f32), pltpu.SMEM((total,), jnp.int32)],
            name="align",
        )(owner, block_slot, got)
        aligned = exchange(mean)
        asked = got
    else:
        pieces = sharer_values.reshape(blocks, devices, slice_len * width).transpose(1, 0, 2)
        got = exchange(pieces).reshape(total, slice_len * width)
        dest = owner * blocks + block_slot
        hot = (dest[None, :] == jnp.arange(total, dtype=jnp.int32)[:, None]).astype(bf16)
        sums = jnp.dot(hot, got, preferred_element_type=f32)
        count = jnp.sum(hot.astype(f32), axis=1, keepdims=True)
        mean = (sums / jnp.maximum(count, 1.0)).astype(bf16)
        aligned = exchange(mean.reshape(devices, blocks, slice_len * width))
        aligned = aligned.reshape(devices, blocks, slice_len, width).transpose(1, 0, 2, 3)
        aligned = aligned.reshape(tokens, width)
        asked = lax.all_gather(queries.reshape(1, heads * G, DH), "ctx", axis=0, tiled=True)

    weights, part = pl.pallas_call(
        functools.partial(score_kernel, heads=heads),
        out_shape=(
            shape((heads, rows * G, tokens), bf16),
            shape((rows, heads * G + STAT, DH), f32),
        ),
        in_specs=[SMEM, VMEM, VMEM, VMEM, VMEM],
        cost_estimate=pl.CostEstimate(
            flops=2 * heads * rows * G * tokens * DH,
            bytes_accessed=2 * 10**6,
            transcendentals=heads * rows * G * tokens,
        ),
        name="score",
    )(place, asked, recv_keys, new_keys, new_values)
    merged, numer = pl.pallas_call(
        functools.partial(
            mixer_kernel, blocks=blocks, slice_len=slice_len if tiled else 0, chunk=512
        ),
        out_shape=(shape((tokens, width), bf16), shape(part.shape, f32)),
        in_specs=[SMEM] + [VMEM] * 7,
        name="mixer",
    )(gate_logit, aligned, recv_values, mixer_gate, mixer_up, mixer_down, weights, part)
    attended = pl.pallas_call(
        functools.partial(combine_kernel, heads=heads),
        out_shape=shape((1, heads * G * DH), bf16),
        scratch_shapes=[pltpu.VMEM((heads * G, DH), f32)],
        name="combine",
    )(exchange(numer))
    return merged, attended


def solution(mesh):
    rows = P(("grp", "ctx"), "head")
    return jax.shard_map(
        body,
        mesh=mesh,
        in_specs=(P("grp", None), P("grp"), rows, rows, rows, rows, rows, rows, P(), P(), P(), P("head")),
        out_specs=(rows, rows),
        check_vma=False,
    )
```

```python
import functools
import math

import jax
import jax.numpy as jnp
from jax import lax
from jax.experimental import pallas as pl
from jax.experimental.pallas import tpu as pltpu
from jax.sharding import PartitionSpec as P

DH = 128
BLK = 128
G = 8
STAT = 8
NEG = -1e30
SMEM = pl.BlockSpec(memory_space=pltpu.SMEM)
VMEM = pl.BlockSpec(memory_space=pltpu.VMEM)
ANY = pl.BlockSpec(memory_space=pl.ANY)


def exchange(x):
    return lax.all_to_all(x, "ctx", split_axis=0, concat_axis=0, tiled=True)


def query_tile(query_ref, scratch):
    for r in range(scratch.shape[0]):
        scratch[r : r + 1, :] = query_ref[0:1, r * DH : (r + 1) * DH].astype(jnp.float32)
    return scratch[...].astype(jnp.bfloat16)


def pack_kernel(sharer_ref, query_ref, out_ref, scratch, *, blocks, slice_len):
    devices = out_ref.shape[0]
    width = sharer_ref.shape[1]
    q = query_tile(query_ref, scratch)
    for d in range(devices):
        for k in range(blocks):
            start = k * BLK + d * slice_len
            out_ref[d, k * slice_len : (k + 1) * slice_len, :width] = sharer_ref[
                start : start + slice_len, :
            ]
        out_ref[d, :, width:] = q


def align_kernel(owner_ref, slot_ref, got_ref, out_ref, sums, counts, *, blocks, slice_len):
    devices = out_ref.shape[0]
    width = out_ref.shape[2]
    total = devices * blocks
    sums[...] = jnp.zeros(sums.shape, jnp.float32)
    for r in range(total):
        counts[r] = 0
    for b in range(total):
        dest = owner_ref[b] * blocks + slot_ref[b]
        s, k = divmod(b, blocks)
        sums[dest] += got_ref[s, k * slice_len : (k + 1) * slice_len, :width].astype(jnp.float32)
        counts[dest] = counts[dest] + 1
    for r in range(total):
        d, k = divmod(r, blocks)
        many = jnp.full((1, width), jnp.maximum(counts[r], 1), jnp.int32).astype(jnp.float32)
        out_ref[d, k * slice_len : (k + 1) * slice_len, :] = (sums[r] / many).astype(jnp.bfloat16)


def score_kernel(
    place_ref, got_ref, key_ref, new_key_ref, new_value_ref, gate_hbm, up_hbm, down_hbm,
    weight_ref, part_ref, gate_ref, up_ref, down_ref, sems, *, heads
):
    pairs = ((gate_hbm, gate_ref), (up_hbm, up_ref), (down_hbm, down_ref))
    copies = [pltpu.make_async_copy(a, b, sems.at[i]) for i, (a, b) in enumerate(pairs)]
    for copy in copies:
        copy.start()
    rows = got_ref.shape[0]
    scale = 1.0 / math.sqrt(DH)
    q_all = got_ref[:, :, got_ref.shape[2] - DH :].astype(jnp.float32)
    row_of = lax.broadcasted_iota(jnp.int32, (rows * G, 1), 0) // G
    allowed = row_of >= place_ref[0]
    sub = lax.broadcasted_iota(jnp.int32, (1, G, DH), 1)
    lane = lax.broadcasted_iota(jnp.int32, (1, G, DH), 2)
    tops = jnp.zeros((rows, 1, DH), jnp.float32)
    dens = jnp.zeros((rows, 1, DH), jnp.float32)
    for j in range(heads):
        cols = slice(j * DH, (j + 1) * DH)
        q = q_all[:, j * G : (j + 1) * G, :].reshape(rows * G, DH)
        s = (
            lax.dot_general(
                q.astype(jnp.bfloat16),
                key_ref[:, cols],
                (((1,), (1,)), ((), ())),
                preferred_element_type=jnp.float32,
            )
            * scale
        )
        sf = jnp.sum(q * new_key_ref[0:1, cols].astype(jnp.float32), axis=1, keepdims=True) * scale
        top = jnp.maximum(
            jnp.max(s, axis=1, keepdims=True), jnp.where(allowed, sf, NEG)
        )
        w = jnp.exp(s - top)
        wf = jnp.where(allowed, jnp.exp(jnp.where(allowed, sf, top) - top), 0.0)
        den = jnp.sum(w, axis=1, keepdims=True) + wf
        weight_ref[j] = w.astype(jnp.bfloat16)
        fresh = wf.astype(jnp.bfloat16).astype(jnp.float32) * new_value_ref[0:1, cols].astype(
            jnp.float32
        )
        part_ref[:, j * G : (j + 1) * G, :] = fresh.reshape(rows, G, DH)
        here = lane == sub + j * G
        spread = lambda v: jnp.sum(
            jnp.where(here, jnp.broadcast_to(v, (rows * G, DH)).reshape(rows, G, DH), 0.0),
            axis=1,
            keepdims=True,
        )
        tops += spread(top)
        dens += spread(den)
    part_ref[:, heads * G :, :] = jnp.where(
        sub == 0, jnp.broadcast_to(tops, (rows, STAT, DH)), jnp.broadcast_to(dens, (rows, STAT, DH))
    )
    for copy in copies:
        copy.wait()


def mixer_kernel(
    logit_ref, got_ref, value_ref, gate_ref, up_ref, down_ref, weight_ref, part_ref, merged_ref, out_ref,
    *, blocks, slice_len
):
    tokens, width = value_ref.shape
    heads = width // DH
    rows = part_ref.shape[0]
    out_ref[:, heads * G :, :] = part_ref[:, heads * G :, :]
    updates = []
    for first in range(0, heads, 2):
        joined = []
        for j in range(first, first + 2):
            cols = slice(j * DH, (j + 1) * DH)
            if slice_len:
                a = jnp.concatenate(
                    [
                        got_ref[s, k * slice_len : (k + 1) * slice_len, cols]
                        for k in range(blocks)
                        for s in range(got_ref.shape[0])
                    ],
                    axis=0,
                )
            else:
                a = got_ref[:, cols]
            joined.append(jnp.concatenate([value_ref[:, cols], a], axis=1))
        x = jnp.concatenate(joined, axis=0)
        g = jnp.dot(x, gate_ref[...], preferred_element_type=jnp.float32)
        u = jnp.dot(x, up_ref[...], preferred_element_type=jnp.float32)
        half = g * 0.5
        h = ((half + half * jnp.tanh(half)) * u).astype(jnp.bfloat16)
        updates.append(jnp.dot(h, down_ref[...], preferred_element_type=jnp.float32))
    for j in range(heads):
        cols = slice(j * DH, (j + 1) * DH)
        update = updates[j // 2][(j % 2) * tokens : (j % 2 + 1) * tokens]
        head_gate = jax.nn.sigmoid(jnp.full((1, DH), logit_ref[j], jnp.float32))
        merged = (value_ref[:, cols].astype(jnp.float32) + head_gate * update).astype(jnp.bfloat16)
        merged_ref[:, cols] = merged
        numer = jnp.dot(weight_ref[j], merged, preferred_element_type=jnp.float32)
        out_ref[:, j * G : (j + 1) * G, :] = part_ref[:, j * G : (j + 1) * G, :] + numer.reshape(
            rows, G, DH
        )


def combine_kernel(got_ref, out_ref, scratch, *, heads):
    n = heads * G
    tops = got_ref[:, n : n + 1, :]
    dens = got_ref[:, n + 1 : n + 2, :]
    factor = jnp.exp(tops - jnp.max(tops, axis=0, keepdims=True))
    factor = factor / jnp.sum(factor * dens, axis=0, keepdims=True)
    sub = lax.broadcasted_iota(jnp.int32, (1, n, DH), 1)
    lane = lax.broadcasted_iota(jnp.int32, (1, n, DH), 2)
    column = jnp.sum(jnp.where(lane == sub, factor, 0.0), axis=2, keepdims=True)
    scratch[...] = jnp.sum(column * got_ref[:, :n, :], axis=0)
    for r in range(n):
        out_ref[0:1, r * DH : (r + 1) * DH] = scratch[r : r + 1, :].astype(jnp.bfloat16)


def body(
    block_owner, block_slot, recv_keys, recv_values, sharer_values, queries, new_keys, new_values,
    mixer_gate, mixer_up, mixer_down, gate_logit,
):
    devices = lax.axis_size("ctx")
    place = lax.axis_index("ctx").astype(jnp.int32).reshape(1)
    tokens, width = recv_values.shape
    heads = width // DH
    blocks = tokens // BLK
    total = blocks * devices
    slice_len = BLK // devices
    owner = block_owner[:, 0]
    rows = devices
    tiled = slice_len % 16 == 0
    f32, bf16 = jnp.float32, jnp.bfloat16
    shape = jax.ShapeDtypeStruct
    near = pltpu.VMEM if tiled else shape

    def here(x):
        return pltpu.with_memory_space_constraint(x, pltpu.VMEM) if tiled else x

    if tiled:
        send = pl.pallas_call(
            functools.partial(pack_kernel, blocks=blocks, slice_len=slice_len),
            out_shape=shape((devices, blocks * slice_len, width + DH), bf16),
            scratch_shapes=[pltpu.VMEM((heads * G, DH), f32)],
            name="pack",
        )(sharer_values, queries)
        got = here(exchange(send))
        mean = pl.pallas_call(
            functools.partial(align_kernel, blocks=blocks, slice_len=slice_len),
            out_shape=shape((devices, blocks * slice_len, width), bf16),
            in_specs=[SMEM, SMEM, VMEM],
            scratch_shapes=[pltpu.VMEM((total, slice_len, width), f32), pltpu.SMEM((total,), jnp.int32)],
            name="align",
        )(owner, block_slot, got)
        aligned = exchange(mean)
        asked = got
    else:
        pieces = sharer_values.reshape(blocks, devices, slice_len * width).transpose(1, 0, 2)
        got = exchange(pieces).reshape(total, slice_len * width)
        dest = owner * blocks + block_slot
        hot = (dest[None, :] == jnp.arange(total, dtype=jnp.int32)[:, None]).astype(bf16)
        sums = jnp.dot(hot, got, preferred_element_type=f32)
        count = jnp.sum(hot.astype(f32), axis=1, keepdims=True)
        mean = (sums / jnp.maximum(count, 1.0)).astype(bf16)
        aligned = exchange(mean.reshape(devices, blocks, slice_len * width))
        aligned = aligned.reshape(devices, blocks, slice_len, width).transpose(1, 0, 2, 3)
        aligned = aligned.reshape(tokens, width)
        asked = lax.all_gather(queries.reshape(1, heads * G, DH), "ctx", axis=0, tiled=True)

    weights, part, gate_v, up_v, down_v = pl.pallas_call(
        functools.partial(score_kernel, heads=heads),
        out_shape=(
            shape((heads, rows * G, tokens), bf16),
            shape((rows, heads * G + STAT, DH), f32),
            near(mixer_gate.shape, bf16),
            near(mixer_up.shape, bf16),
            near(mixer_down.shape, bf16),
        ),
        in_specs=[SMEM] + [VMEM] * 4 + [ANY] * 3,
        scratch_shapes=[pltpu.SemaphoreType.DMA((3,))],
        cost_estimate=pl.CostEstimate(
            flops=2 * heads * rows * G * tokens * DH,
            bytes_accessed=2 * 10**6,
            transcendentals=heads * rows * G * tokens,
        ),
        name="score",
    )(
        place, asked, recv_keys, new_keys, new_values, mixer_gate, mixer_up, mixer_down
    )
    merged, numer = pl.pallas_call(
        functools.partial(mixer_kernel, blocks=blocks, slice_len=slice_len if tiled else 0),
        out_shape=(shape((tokens, width), bf16), shape(part.shape, f32)),
        in_specs=[SMEM] + [VMEM] * 7,
        name="mixer",
    )(
        gate_logit, here(aligned), recv_values, here(gate_v), here(up_v), here(down_v),
        weights, part,
    )
    attended = pl.pallas_call(
        functools.partial(combine_kernel, heads=heads),
        out_shape=shape((1, heads * G * DH), bf16),
        scratch_shapes=[pltpu.VMEM((heads * G, DH), f32)],
        name="combine",
    )(here(exchange(numer)))
    return merged, attended


def solution(mesh):
    rows = P(("grp", "ctx"), "head")
    return jax.shard_map(
        body,
        mesh=mesh,
        in_specs=(P("grp", None), P("grp"), rows, rows, rows, rows, rows, rows, P(), P(), P(), P("head")),
        out_specs=(rows, rows),
        check_vma=False,
    )
```

```python
import functools
import math

import jax
import jax.numpy as jnp
from jax import lax
from jax.experimental import pallas as pl
from jax.experimental.pallas import tpu as pltpu
from jax.sharding import PartitionSpec as P

DH = 128
BLK = 128
G = 8
STAT = 8
NEG = -1e30
SMEM = pl.BlockSpec(memory_space=pltpu.SMEM)
VMEM = pl.BlockSpec(memory_space=pltpu.VMEM)
ANY = pl.BlockSpec(memory_space=pl.ANY)


def exchange(x):
    return lax.all_to_all(x, "ctx", split_axis=0, concat_axis=0, tiled=True)


def query_tile(query_ref, scratch):
    for r in range(scratch.shape[0]):
        scratch[r : r + 1, :] = query_ref[0:1, r * DH : (r + 1) * DH].astype(jnp.float32)
    return scratch[...].astype(jnp.bfloat16)


def pack_kernel(sharer_hbm, query_ref, out_ref, scratch, sems, *, blocks, slice_len):
    devices = out_ref.shape[0]
    width = sharer_hbm.shape[1]
    copies = []
    for d in range(devices):
        for k in range(blocks):
            copies.append(
                pltpu.make_async_copy(
                    sharer_hbm.at[pl.ds(k * BLK + d * slice_len, slice_len), :],
                    out_ref.at[d, pl.ds(k * slice_len, slice_len), pl.ds(0, width)],
                    sems.at[d, k],
                )
            )
            copies[-1].start()
    q = query_tile(query_ref, scratch)
    for d in range(devices):
        out_ref[d, :, width:] = q
    for copy in copies:
        copy.wait()


def align_kernel(owner_ref, slot_ref, got_ref, out_ref, sums, counts, *, blocks, slice_len):
    devices = out_ref.shape[0]
    width = out_ref.shape[2]
    total = devices * blocks
    sums[...] = jnp.zeros(sums.shape, jnp.float32)
    for r in range(total):
        counts[r] = 0
    for b in range(total):
        dest = owner_ref[b] * blocks + slot_ref[b]
        s, k = divmod(b, blocks)
        sums[dest] += got_ref[s, k * slice_len : (k + 1) * slice_len, :width].astype(jnp.float32)
        counts[dest] = counts[dest] + 1
    for r in range(total):
        d, k = divmod(r, blocks)
        many = jnp.full((1, width), jnp.maximum(counts[r], 1), jnp.int32).astype(jnp.float32)
        out_ref[d, k * slice_len : (k + 1) * slice_len, :] = (sums[r] / many).astype(jnp.bfloat16)


def score_kernel(
    place_ref, got_ref, key_ref, new_key_ref, new_value_ref, gate_hbm, up_hbm, down_hbm,
    weight_ref, part_ref, gate_ref, up_ref, down_ref, sems, *, heads
):
    pairs = ((gate_hbm, gate_ref), (up_hbm, up_ref), (down_hbm, down_ref))
    copies = [pltpu.make_async_copy(a, b, sems.at[i]) for i, (a, b) in enumerate(pairs)]
    for copy in copies:
        copy.start()
    rows = got_ref.shape[0]
    scale = 1.0 / math.sqrt(DH)
    q_all = got_ref[:, :, got_ref.shape[2] - DH :].astype(jnp.float32)
    row_of = lax.broadcasted_iota(jnp.int32, (rows * G, 1), 0) // G
    allowed = row_of >= place_ref[0]
    sub = lax.broadcasted_iota(jnp.int32, (1, G, DH), 1)
    lane = lax.broadcasted_iota(jnp.int32, (1, G, DH), 2)
    tops = jnp.zeros((rows, 1, DH), jnp.float32)
    dens = jnp.zeros((rows, 1, DH), jnp.float32)
    for j in range(heads):
        cols = slice(j * DH, (j + 1) * DH)
        q = q_all[:, j * G : (j + 1) * G, :].reshape(rows * G, DH)
        s = (
            lax.dot_general(
                q.astype(jnp.bfloat16),
                key_ref[:, cols],
                (((1,), (1,)), ((), ())),
                preferred_element_type=jnp.float32,
            )
            * scale
        )
        sf = jnp.sum(q * new_key_ref[0:1, cols].astype(jnp.float32), axis=1, keepdims=True) * scale
        top = jnp.maximum(
            jnp.max(s, axis=1, keepdims=True), jnp.where(allowed, sf, NEG)
        )
        w = jnp.exp(s - top)
        wf = jnp.where(allowed, jnp.exp(jnp.where(allowed, sf, top) - top), 0.0)
        den = jnp.sum(w, axis=1, keepdims=True) + wf
        weight_ref[j] = w.astype(jnp.bfloat16)
        fresh = wf.astype(jnp.bfloat16).astype(jnp.float32) * new_value_ref[0:1, cols].astype(
            jnp.float32
        )
        part_ref[:, j * G : (j + 1) * G, :] = fresh.reshape(rows, G, DH)
        here = lane == sub + j * G
        spread = lambda v: jnp.sum(
            jnp.where(here, jnp.broadcast_to(v, (rows * G, DH)).reshape(rows, G, DH), 0.0),
            axis=1,
            keepdims=True,
        )
        tops += spread(top)
        dens += spread(den)
    part_ref[:, heads * G :, :] = jnp.where(
        sub == 0, jnp.broadcast_to(tops, (rows, STAT, DH)), jnp.broadcast_to(dens, (rows, STAT, DH))
    )
    for copy in copies:
        copy.wait()


def mixer_kernel(
    logit_ref, got_ref, value_ref, gate_ref, up_ref, down_ref, weight_ref, part_ref, merged_ref, out_ref,
    *, blocks, slice_len
):
    tokens, width = value_ref.shape
    heads = width // DH
    rows = part_ref.shape[0]
    out_ref[:, heads * G :, :] = part_ref[:, heads * G :, :]
    updates = []
    for first in range(0, heads, 2):
        joined = []
        for j in range(first, first + 2):
            cols = slice(j * DH, (j + 1) * DH)
            if slice_len:
                a = jnp.concatenate(
                    [
                        got_ref[s, k * slice_len : (k + 1) * slice_len, cols]
                        for k in range(blocks)
                        for s in range(got_ref.shape[0])
                    ],
                    axis=0,
                )
            else:
                a = got_ref[:, cols]
            joined.append(jnp.concatenate([value_ref[:, cols], a], axis=1))
        x = jnp.concatenate(joined, axis=0)
        g = jnp.dot(x, gate_ref[...], preferred_element_type=jnp.float32)
        u = jnp.dot(x, up_ref[...], preferred_element_type=jnp.float32)
        half = g * 0.5
        h = ((half + half * jnp.tanh(half)) * u).astype(jnp.bfloat16)
        updates.append(jnp.dot(h, down_ref[...], preferred_element_type=jnp.float32))
    for j in range(heads):
        cols = slice(j * DH, (j + 1) * DH)
        update = updates[j // 2][(j % 2) * tokens : (j % 2 + 1) * tokens]
        head_gate = jax.nn.sigmoid(jnp.full((1, DH), logit_ref[j], jnp.float32))
        merged = (value_ref[:, cols].astype(jnp.float32) + head_gate * update).astype(jnp.bfloat16)
        merged_ref[:, cols] = merged
        numer = jnp.dot(weight_ref[j], merged, preferred_element_type=jnp.float32)
        out_ref[:, j * G : (j + 1) * G, :] = part_ref[:, j * G : (j + 1) * G, :] + numer.reshape(
            rows, G, DH
        )


def combine_kernel(got_ref, out_ref, scratch, *, heads):
    n = heads * G
    tops = got_ref[:, n : n + 1, :]
    dens = got_ref[:, n + 1 : n + 2, :]
    factor = jnp.exp(tops - jnp.max(tops, axis=0, keepdims=True))
    factor = factor / jnp.sum(factor * dens, axis=0, keepdims=True)
    sub = lax.broadcasted_iota(jnp.int32, (1, n, DH), 1)
    lane = lax.broadcasted_iota(jnp.int32, (1, n, DH), 2)
    column = jnp.sum(jnp.where(lane == sub, factor, 0.0), axis=2, keepdims=True)
    scratch[...] = jnp.sum(column * got_ref[:, :n, :], axis=0)
    for r in range(n):
        out_ref[0:1, r * DH : (r + 1) * DH] = scratch[r : r + 1, :].astype(jnp.bfloat16)


def body(
    block_owner, block_slot, recv_keys, recv_values, sharer_values, queries, new_keys, new_values,
    mixer_gate, mixer_up, mixer_down, gate_logit,
):
    devices = lax.axis_size("ctx")
    place = lax.axis_index("ctx").astype(jnp.int32).reshape(1)
    tokens, width = recv_values.shape
    heads = width // DH
    blocks = tokens // BLK
    total = blocks * devices
    slice_len = BLK // devices
    owner = block_owner[:, 0]
    rows = devices
    tiled = slice_len % 16 == 0
    f32, bf16 = jnp.float32, jnp.bfloat16
    shape = jax.ShapeDtypeStruct
    near = pltpu.VMEM if tiled else shape

    def here(x):
        return pltpu.with_memory_space_constraint(x, pltpu.VMEM) if tiled else x

    if tiled:
        send = pl.pallas_call(
            functools.partial(pack_kernel, blocks=blocks, slice_len=slice_len),
            out_shape=near((devices, blocks * slice_len, width + DH), bf16),
            in_specs=[ANY, VMEM],
            scratch_shapes=[
                pltpu.VMEM((heads * G, DH), f32),
                pltpu.SemaphoreType.DMA((devices, blocks)),
            ],
            name="pack",
        )(sharer_values, queries)
        got = here(exchange(send))
        mean = pl.pallas_call(
            functools.partial(align_kernel, blocks=blocks, slice_len=slice_len),
            out_shape=near((devices, blocks * slice_len, width), bf16),
            in_specs=[SMEM, SMEM, VMEM],
            scratch_shapes=[pltpu.VMEM((total, slice_len, width), f32), pltpu.SMEM((total,), jnp.int32)],
            name="align",
        )(owner, block_slot, got)
        aligned = exchange(mean)
        asked = got
    else:
        pieces = sharer_values.reshape(blocks, devices, slice_len * width).transpose(1, 0, 2)
        got = exchange(pieces).reshape(total, slice_len * width)
        dest = owner * blocks + block_slot
        hot = (dest[None, :] == jnp.arange(total, dtype=jnp.int32)[:, None]).astype(bf16)
        sums = jnp.dot(hot, got, preferred_element_type=f32)
        count = jnp.sum(hot.astype(f32), axis=1, keepdims=True)
        mean = (sums / jnp.maximum(count, 1.0)).astype(bf16)
        aligned = exchange(mean.reshape(devices, blocks, slice_len * width))
        aligned = aligned.reshape(devices, blocks, slice_len, width).transpose(1, 0, 2, 3)
        aligned = aligned.reshape(tokens, width)
        asked = lax.all_gather(queries.reshape(1, heads * G, DH), "ctx", axis=0, tiled=True)

    weights, part, gate_v, up_v, down_v = pl.pallas_call(
        functools.partial(score_kernel, heads=heads),
        out_shape=(
            shape((heads, rows * G, tokens), bf16),
            shape((rows, heads * G + STAT, DH), f32),
            near(mixer_gate.shape, bf16),
            near(mixer_up.shape, bf16),
            near(mixer_down.shape, bf16),
        ),
        in_specs=[SMEM] + [VMEM] * 4 + [ANY] * 3,
        scratch_shapes=[pltpu.SemaphoreType.DMA((3,))],
        cost_estimate=pl.CostEstimate(
            flops=2 * heads * rows * G * tokens * DH,
            bytes_accessed=2 * 10**6,
            transcendentals=heads * rows * G * tokens,
        ),
        name="score",
    )(
        place, asked, recv_keys, new_keys, new_values, mixer_gate, mixer_up, mixer_down
    )
    merged, numer = pl.pallas_call(
        functools.partial(mixer_kernel, blocks=blocks, slice_len=slice_len if tiled else 0),
        out_shape=(shape((tokens, width), bf16), near(part.shape, f32)),
        in_specs=[SMEM] + [VMEM] * 7,
        name="mixer",
    )(
        gate_logit, here(aligned), recv_values, here(gate_v), here(up_v), here(down_v),
        weights, part,
    )
    attended = pl.pallas_call(
        functools.partial(combine_kernel, heads=heads),
        out_shape=shape((1, heads * G * DH), bf16),
        scratch_shapes=[pltpu.VMEM((heads * G, DH), f32)],
        name="combine",
    )(here(exchange(numer)))
    return merged, attended


def solution(mesh):
    rows = P(("grp", "ctx"), "head")
    return jax.shard_map(
        body,
        mesh=mesh,
        in_specs=(P("grp", None), P("grp"), rows, rows, rows, rows, rows, rows, P(), P(), P(), P("head")),
        out_specs=(rows, rows),
        check_vma=False,
    )
```

```python
import functools
import math

import jax
import jax.numpy as jnp
from jax import lax
from jax.experimental import pallas as pl
from jax.experimental.pallas import tpu as pltpu
from jax.sharding import PartitionSpec as P

DH = 128
BLK = 128
G = 8
STAT = 8
NEG = -1e30
SMEM = pl.BlockSpec(memory_space=pltpu.SMEM)
VMEM = pl.BlockSpec(memory_space=pltpu.VMEM)
ANY = pl.BlockSpec(memory_space=pl.ANY)


def exchange(x):
    return lax.all_to_all(x, "ctx", split_axis=0, concat_axis=0, tiled=True)


def query_tile(query_ref, scratch):
    for r in range(scratch.shape[0]):
        scratch[r : r + 1, :] = query_ref[0:1, r * DH : (r + 1) * DH].astype(jnp.float32)
    return scratch[...].astype(jnp.bfloat16)


def pack_kernel(sharer_hbm, query_hbm, out_ref, query_ref, scratch, sems, query_sem, *, blocks, slice_len):
    devices = out_ref.shape[0]
    query_copy = pltpu.make_async_copy(query_hbm, query_ref, query_sem)
    query_copy.start()
    width = sharer_hbm.shape[1]
    copies = []
    for d in range(devices):
        for k in range(blocks):
            copies.append(
                pltpu.make_async_copy(
                    sharer_hbm.at[pl.ds(k * BLK + d * slice_len, slice_len), :],
                    out_ref.at[d, pl.ds(k * slice_len, slice_len), pl.ds(0, width)],
                    sems.at[d, k],
                )
            )
            copies[-1].start()
    query_copy.wait()
    q = query_tile(query_ref, scratch)
    for d in range(devices):
        out_ref[d, :, width:] = q
    for copy in copies:
        copy.wait()


def align_kernel(owner_ref, slot_ref, got_ref, out_ref, sums, counts, *, blocks, slice_len):
    devices = out_ref.shape[0]
    width = out_ref.shape[2]
    total = devices * blocks
    sums[...] = jnp.zeros(sums.shape, jnp.float32)
    for r in range(total):
        counts[r] = 0
    for b in range(total):
        dest = owner_ref[b] * blocks + slot_ref[b]
        s, k = divmod(b, blocks)
        sums[dest] += got_ref[s, k * slice_len : (k + 1) * slice_len, :width].astype(jnp.float32)
        counts[dest] = counts[dest] + 1
    for r in range(total):
        d, k = divmod(r, blocks)
        many = jnp.full((1, width), jnp.maximum(counts[r], 1), jnp.int32).astype(jnp.float32)
        out_ref[d, k * slice_len : (k + 1) * slice_len, :] = (sums[r] / many).astype(jnp.bfloat16)


def score_kernel(
    place_ref, got_ref, key_ref, new_key_ref, new_value_ref, gate_hbm, up_hbm, down_hbm,
    weight_ref, part_ref, gate_ref, up_ref, down_ref, sems, *, heads
):
    pairs = ((gate_hbm, gate_ref), (up_hbm, up_ref), (down_hbm, down_ref))
    copies = [pltpu.make_async_copy(a, b, sems.at[i]) for i, (a, b) in enumerate(pairs)]
    for copy in copies:
        copy.start()
    rows = got_ref.shape[0]
    scale = 1.0 / math.sqrt(DH)
    q_all = got_ref[:, :, got_ref.shape[2] - DH :].astype(jnp.float32)
    row_of = lax.broadcasted_iota(jnp.int32, (rows * G, 1), 0) // G
    allowed = row_of >= place_ref[0]
    sub = lax.broadcasted_iota(jnp.int32, (1, G, DH), 1)
    lane = lax.broadcasted_iota(jnp.int32, (1, G, DH), 2)
    tops = jnp.zeros((rows, 1, DH), jnp.float32)
    dens = jnp.zeros((rows, 1, DH), jnp.float32)
    for j in range(heads):
        cols = slice(j * DH, (j + 1) * DH)
        q = q_all[:, j * G : (j + 1) * G, :].reshape(rows * G, DH)
        s = (
            lax.dot_general(
                q.astype(jnp.bfloat16),
                key_ref[:, cols],
                (((1,), (1,)), ((), ())),
                preferred_element_type=jnp.float32,
            )
            * scale
        )
        sf = jnp.sum(q * new_key_ref[0:1, cols].astype(jnp.float32), axis=1, keepdims=True) * scale
        top = jnp.maximum(
            jnp.max(s, axis=1, keepdims=True), jnp.where(allowed, sf, NEG)
        )
        w = jnp.exp(s - top)
        wf = jnp.where(allowed, jnp.exp(jnp.where(allowed, sf, top) - top), 0.0)
        den = jnp.sum(w, axis=1, keepdims=True) + wf
        weight_ref[j] = w.astype(jnp.bfloat16)
        fresh = wf.astype(jnp.bfloat16).astype(jnp.float32) * new_value_ref[0:1, cols].astype(
            jnp.float32
        )
        part_ref[:, j * G : (j + 1) * G, :] = fresh.reshape(rows, G, DH)
        here = lane == sub + j * G
        spread = lambda v: jnp.sum(
            jnp.where(here, jnp.broadcast_to(v, (rows * G, DH)).reshape(rows, G, DH), 0.0),
            axis=1,
            keepdims=True,
        )
        tops += spread(top)
        dens += spread(den)
    part_ref[:, heads * G :, :] = jnp.where(
        sub == 0, jnp.broadcast_to(tops, (rows, STAT, DH)), jnp.broadcast_to(dens, (rows, STAT, DH))
    )
    for copy in copies:
        copy.wait()


def mixer_kernel(
    logit_ref, got_ref, value_ref, gate_ref, up_ref, down_ref, weight_ref, part_ref, merged_hbm, out_ref,
    merged_ref, sems, *, blocks, slice_len
):
    tokens, width = value_ref.shape
    heads = width // DH
    rows = part_ref.shape[0]
    out_ref[:, heads * G :, :] = part_ref[:, heads * G :, :]
    copies = []
    for first in range(0, heads, 2):
        joined = []
        for j in range(first, first + 2):
            cols = slice(j * DH, (j + 1) * DH)
            if slice_len:
                a = jnp.concatenate(
                    [
                        got_ref[s, k * slice_len : (k + 1) * slice_len, cols]
                        for k in range(blocks)
                        for s in range(got_ref.shape[0])
                    ],
                    axis=0,
                )
            else:
                a = got_ref[:, cols]
            joined.append(jnp.concatenate([value_ref[:, cols], a], axis=1))
        x = jnp.concatenate(joined, axis=0)
        g = jnp.dot(x, gate_ref[...], preferred_element_type=jnp.float32)
        u = jnp.dot(x, up_ref[...], preferred_element_type=jnp.float32)
        half = g * 0.5
        h = ((half + half * jnp.tanh(half)) * u).astype(jnp.bfloat16)
        updates = jnp.dot(h, down_ref[...], preferred_element_type=jnp.float32)
        for j in range(first, first + 2):
            cols = slice(j * DH, (j + 1) * DH)
            update = updates[(j - first) * tokens : (j - first + 1) * tokens]
            head_gate = jax.nn.sigmoid(jnp.full((1, DH), logit_ref[j], jnp.float32))
            merged = (value_ref[:, cols].astype(jnp.float32) + head_gate * update).astype(jnp.bfloat16)
            merged_ref[:, cols] = merged
            head = pl.ds(j * DH, DH)
            copies.append(
                pltpu.make_async_copy(merged_ref.at[:, head], merged_hbm.at[:, head], sems.at[j])
            )
            copies[-1].start()
            numer = jnp.dot(weight_ref[j], merged, preferred_element_type=jnp.float32)
            out_ref[:, j * G : (j + 1) * G, :] = part_ref[:, j * G : (j + 1) * G, :] + numer.reshape(
                rows, G, DH
            )
    for copy in copies:
        copy.wait()


def combine_kernel(got_ref, out_ref, scratch, *, heads):
    n = heads * G
    tops = got_ref[:, n : n + 1, :]
    dens = got_ref[:, n + 1 : n + 2, :]
    factor = jnp.exp(tops - jnp.max(tops, axis=0, keepdims=True))
    factor = factor / jnp.sum(factor * dens, axis=0, keepdims=True)
    sub = lax.broadcasted_iota(jnp.int32, (1, n, DH), 1)
    lane = lax.broadcasted_iota(jnp.int32, (1, n, DH), 2)
    column = jnp.sum(jnp.where(lane == sub, factor, 0.0), axis=2, keepdims=True)
    scratch[...] = jnp.sum(column * got_ref[:, :n, :], axis=0)
    for r in range(n):
        out_ref[0:1, r * DH : (r + 1) * DH] = scratch[r : r + 1, :].astype(jnp.bfloat16)


def body(
    block_owner, block_slot, recv_keys, recv_values, sharer_values, queries, new_keys, new_values,
    mixer_gate, mixer_up, mixer_down, gate_logit,
):
    devices = lax.axis_size("ctx")
    place = lax.axis_index("ctx").astype(jnp.int32).reshape(1)
    tokens, width = recv_values.shape
    heads = width // DH
    blocks = tokens // BLK
    total = blocks * devices
    slice_len = BLK // devices
    owner = block_owner[:, 0]
    rows = devices
    tiled = slice_len % 16 == 0
    f32, bf16 = jnp.float32, jnp.bfloat16
    shape = jax.ShapeDtypeStruct
    near = pltpu.VMEM if tiled else shape

    def here(x):
        return pltpu.with_memory_space_constraint(x, pltpu.VMEM) if tiled else x

    if tiled:
        send = pl.pallas_call(
            functools.partial(pack_kernel, blocks=blocks, slice_len=slice_len),
            out_shape=near((devices, blocks * slice_len, width + DH), bf16),
            in_specs=[ANY, ANY],
            scratch_shapes=[
                pltpu.VMEM(queries.shape, bf16),
                pltpu.VMEM((heads * G, DH), f32),
                pltpu.SemaphoreType.DMA((devices, blocks)),
                pltpu.SemaphoreType.DMA(()),
            ],
            name="pack",
        )(sharer_values, queries)
        got = here(exchange(send))
        mean = pl.pallas_call(
            functools.partial(align_kernel, blocks=blocks, slice_len=slice_len),
            out_shape=near((devices, blocks * slice_len, width), bf16),
            in_specs=[SMEM, SMEM, VMEM],
            scratch_shapes=[pltpu.VMEM((total, slice_len, width), f32), pltpu.SMEM((total,), jnp.int32)],
            name="align",
        )(owner, block_slot, got)
        aligned = exchange(mean)
        asked = got
    else:
        pieces = sharer_values.reshape(blocks, devices, slice_len * width).transpose(1, 0, 2)
        got = exchange(pieces).reshape(total, slice_len * width)
        dest = owner * blocks + block_slot
        hot = (dest[None, :] == jnp.arange(total, dtype=jnp.int32)[:, None]).astype(bf16)
        sums = jnp.dot(hot, got, preferred_element_type=f32)
        count = jnp.sum(hot.astype(f32), axis=1, keepdims=True)
        mean = (sums / jnp.maximum(count, 1.0)).astype(bf16)
        aligned = exchange(mean.reshape(devices, blocks, slice_len * width))
        aligned = aligned.reshape(devices, blocks, slice_len, width).transpose(1, 0, 2, 3)
        aligned = aligned.reshape(tokens, width)
        asked = lax.all_gather(queries.reshape(1, heads * G, DH), "ctx", axis=0, tiled=True)

    weights, part, gate_v, up_v, down_v = pl.pallas_call(
        functools.partial(score_kernel, heads=heads),
        out_shape=(
            shape((heads, rows * G, tokens), bf16),
            shape((rows, heads * G + STAT, DH), f32),
            near(mixer_gate.shape, bf16),
            near(mixer_up.shape, bf16),
            near(mixer_down.shape, bf16),
        ),
        in_specs=[SMEM] + [VMEM] * 4 + [ANY] * 3,
        scratch_shapes=[pltpu.SemaphoreType.DMA((3,))],
        cost_estimate=pl.CostEstimate(
            flops=2 * heads * rows * G * tokens * DH,
            bytes_accessed=2 * 10**6,
            transcendentals=heads * rows * G * tokens,
        ),
        name="score",
    )(
        place, asked, recv_keys, new_keys, new_values, mixer_gate, mixer_up, mixer_down
    )
    merged, numer = pl.pallas_call(
        functools.partial(mixer_kernel, blocks=blocks, slice_len=slice_len if tiled else 0),
        out_shape=(shape((tokens, width), bf16), near(part.shape, f32)),
        in_specs=[SMEM] + [VMEM] * 7,
        out_specs=(ANY, VMEM),
        scratch_shapes=[
            pltpu.VMEM((tokens, width), bf16),
            pltpu.SemaphoreType.DMA((heads,)),
        ],
        name="mixer",
    )(
        gate_logit, here(aligned), recv_values, here(gate_v), here(up_v), here(down_v),
        weights, part,
    )
    attended = pl.pallas_call(
        functools.partial(combine_kernel, heads=heads),
        out_shape=shape((1, heads * G * DH), bf16),
        scratch_shapes=[pltpu.VMEM((heads * G, DH), f32)],
        name="combine",
    )(here(exchange(numer)))
    return merged, attended


def solution(mesh):
    rows = P(("grp", "ctx"), "head")
    return jax.shard_map(
        body,
        mesh=mesh,
        in_specs=(P("grp", None), P("grp"), rows, rows, rows, rows, rows, rows, P(), P(), P(), P("head")),
        out_specs=(rows, rows),
        check_vma=False,
    )
```

```python
import functools
import math

import jax
import jax.numpy as jnp
from jax import lax
from jax.experimental import pallas as pl
from jax.experimental.pallas import tpu as pltpu
from jax.sharding import PartitionSpec as P

DH = 128
BLK = 128
G = 8
STAT = 8
NEG = -1e30
SMEM = pl.BlockSpec(memory_space=pltpu.SMEM)
VMEM = pl.BlockSpec(memory_space=pltpu.VMEM)
ANY = pl.BlockSpec(memory_space=pl.ANY)


def exchange(x):
    return lax.all_to_all(x, "ctx", split_axis=0, concat_axis=0, tiled=True)


def query_tile(query_ref, scratch):
    for r in range(scratch.shape[0]):
        scratch[r : r + 1, :] = query_ref[0:1, r * DH : (r + 1) * DH].astype(jnp.float32)
    return scratch[...].astype(jnp.bfloat16)


def pack_kernel(sharer_hbm, query_hbm, out_ref, query_ref, scratch, sems, query_sem, *, blocks, slice_len):
    devices = out_ref.shape[0]
    query_copy = pltpu.make_async_copy(query_hbm, query_ref, query_sem)
    query_copy.start()
    width = sharer_hbm.shape[1]
    copies = []
    for d in range(devices):
        for k in range(blocks):
            copies.append(
                pltpu.make_async_copy(
                    sharer_hbm.at[pl.ds(k * BLK + d * slice_len, slice_len), :],
                    out_ref.at[d, pl.ds(k * slice_len, slice_len), pl.ds(0, width)],
                    sems.at[d, k],
                )
            )
            copies[-1].start()
    query_copy.wait()
    q = query_tile(query_ref, scratch)
    for d in range(devices):
        out_ref[d, :, width:] = q
    for copy in copies:
        copy.wait()


def align_kernel(
    owner_ref, slot_ref, got_ref, out_hbm, out_ref, sums, counts, sems, *, blocks, slice_len
):
    devices = out_ref.shape[0]
    width = out_ref.shape[2]
    total = devices * blocks
    sums[...] = jnp.zeros(sums.shape, jnp.float32)
    for r in range(total):
        counts[r] = 0
    for b in range(total):
        dest = owner_ref[b] * blocks + slot_ref[b]
        s, k = divmod(b, blocks)
        sums[dest] += got_ref[s, k * slice_len : (k + 1) * slice_len, :width].astype(jnp.float32)
        counts[dest] = counts[dest] + 1
    copies = []
    for r in range(total):
        d, k = divmod(r, blocks)
        many = jnp.full((1, width), jnp.maximum(counts[r], 1), jnp.int32).astype(jnp.float32)
        out_ref[d, k * slice_len : (k + 1) * slice_len, :] = (sums[r] / many).astype(jnp.bfloat16)
        if k == blocks - 1:
            copies.append(pltpu.make_async_copy(out_ref.at[d], out_hbm.at[d], sems.at[d]))
            copies[-1].start()
    for copy in copies:
        copy.wait()


def score_kernel(
    place_ref, got_ref, key_ref, new_key_ref, new_value_ref, gate_hbm, up_hbm, down_hbm,
    weight_ref, part_ref, gate_ref, up_ref, down_ref, sems, *, heads
):
    pairs = ((gate_hbm, gate_ref), (up_hbm, up_ref), (down_hbm, down_ref))
    copies = [pltpu.make_async_copy(a, b, sems.at[i]) for i, (a, b) in enumerate(pairs)]
    for copy in copies:
        copy.start()
    rows = got_ref.shape[0]
    scale = 1.0 / math.sqrt(DH)
    q_all = got_ref[:, :, got_ref.shape[2] - DH :].astype(jnp.float32)
    row_of = lax.broadcasted_iota(jnp.int32, (rows * G, 1), 0) // G
    allowed = row_of >= place_ref[0]
    sub = lax.broadcasted_iota(jnp.int32, (1, G, DH), 1)
    lane = lax.broadcasted_iota(jnp.int32, (1, G, DH), 2)
    tops = jnp.zeros((rows, 1, DH), jnp.float32)
    dens = jnp.zeros((rows, 1, DH), jnp.float32)
    for j in range(heads):
        cols = slice(j * DH, (j + 1) * DH)
        q = q_all[:, j * G : (j + 1) * G, :].reshape(rows * G, DH)
        s = (
            lax.dot_general(
                q.astype(jnp.bfloat16),
                key_ref[:, cols],
                (((1,), (1,)), ((), ())),
                preferred_element_type=jnp.float32,
            )
            * scale
        )
        sf = jnp.sum(q * new_key_ref[0:1, cols].astype(jnp.float32), axis=1, keepdims=True) * scale
        top = jnp.maximum(
            jnp.max(s, axis=1, keepdims=True), jnp.where(allowed, sf, NEG)
        )
        w = jnp.exp(s - top)
        wf = jnp.where(allowed, jnp.exp(jnp.where(allowed, sf, top) - top), 0.0)
        den = jnp.sum(w, axis=1, keepdims=True) + wf
        weight_ref[j] = w.astype(jnp.bfloat16)
        fresh = wf.astype(jnp.bfloat16).astype(jnp.float32) * new_value_ref[0:1, cols].astype(
            jnp.float32
        )
        part_ref[:, j * G : (j + 1) * G, :] = fresh.reshape(rows, G, DH)
        here = lane == sub + j * G
        spread = lambda v: jnp.sum(
            jnp.where(here, jnp.broadcast_to(v, (rows * G, DH)).reshape(rows, G, DH), 0.0),
            axis=1,
            keepdims=True,
        )
        tops += spread(top)
        dens += spread(den)
    part_ref[:, heads * G :, :] = jnp.where(
        sub == 0, jnp.broadcast_to(tops, (rows, STAT, DH)), jnp.broadcast_to(dens, (rows, STAT, DH))
    )
    for copy in copies:
        copy.wait()
    gate_ref[...] = gate_ref[...] * 0.5


def mixer_kernel(
    logit_ref, got_ref, value_ref, gate_ref, up_ref, down_ref, weight_ref, part_ref, merged_ref, out_ref,
    *, blocks, slice_len
):
    heads = value_ref.shape[1] // DH
    rows = part_ref.shape[0]
    out_ref[:, heads * G :, :] = part_ref[:, heads * G :, :]
    updates = []
    for j in range(heads):
        cols = slice(j * DH, (j + 1) * DH)
        if slice_len:
            a = jnp.concatenate(
                [
                    got_ref[s, k * slice_len : (k + 1) * slice_len, cols]
                    for k in range(blocks)
                    for s in range(got_ref.shape[0])
                ],
                axis=0,
            )
        else:
            a = got_ref[:, cols]
        x = jnp.concatenate([value_ref[:, cols], a], axis=1)
        half = jnp.dot(x, gate_ref[...], preferred_element_type=jnp.float32)
        u = jnp.dot(x, up_ref[...], preferred_element_type=jnp.float32)
        h = ((half + half * jnp.tanh(half)) * u).astype(jnp.bfloat16)
        updates.append(jnp.dot(h, down_ref[...], preferred_element_type=jnp.float32))
    for j in range(heads):
        cols = slice(j * DH, (j + 1) * DH)
        head_gate = jax.nn.sigmoid(jnp.full((1, DH), logit_ref[j], jnp.float32))
        merged = (value_ref[:, cols].astype(jnp.float32) + head_gate * updates[j]).astype(jnp.bfloat16)
        merged_ref[:, cols] = merged
        numer = jnp.dot(weight_ref[j], merged, preferred_element_type=jnp.float32)
        out_ref[:, j * G : (j + 1) * G, :] = part_ref[:, j * G : (j + 1) * G, :] + numer.reshape(
            rows, G, DH
        )


def combine_kernel(got_ref, out_ref, scratch, *, heads):
    n = heads * G
    tops = got_ref[:, n : n + 1, :]
    dens = got_ref[:, n + 1 : n + 2, :]
    factor = jnp.exp(tops - jnp.max(tops, axis=0, keepdims=True))
    factor = factor / jnp.sum(factor * dens, axis=0, keepdims=True)
    sub = lax.broadcasted_iota(jnp.int32, (1, n, DH), 1)
    lane = lax.broadcasted_iota(jnp.int32, (1, n, DH), 2)
    column = jnp.sum(jnp.where(lane == sub, factor, 0.0), axis=2, keepdims=True)
    scratch[...] = jnp.sum(column * got_ref[:, :n, :], axis=0)
    for r in range(n):
        out_ref[0:1, r * DH : (r + 1) * DH] = scratch[r : r + 1, :].astype(jnp.bfloat16)


def body(
    block_owner, block_slot, recv_keys, recv_values, sharer_values, queries, new_keys, new_values,
    mixer_gate, mixer_up, mixer_down, gate_logit,
):
    devices = lax.axis_size("ctx")
    place = lax.axis_index("ctx").astype(jnp.int32).reshape(1)
    tokens, width = recv_values.shape
    heads = width // DH
    blocks = tokens // BLK
    total = blocks * devices
    slice_len = BLK // devices
    owner = block_owner[:, 0]
    rows = devices
    tiled = slice_len % 16 == 0
    f32, bf16 = jnp.float32, jnp.bfloat16
    shape = jax.ShapeDtypeStruct
    near = pltpu.VMEM if tiled else shape

    def here(x):
        return pltpu.with_memory_space_constraint(x, pltpu.VMEM) if tiled else x

    if tiled:
        send = pl.pallas_call(
            functools.partial(pack_kernel, blocks=blocks, slice_len=slice_len),
            out_shape=near((devices, blocks * slice_len, width + DH), bf16),
            in_specs=[ANY, ANY],
            scratch_shapes=[
                pltpu.VMEM(queries.shape, bf16),
                pltpu.VMEM((heads * G, DH), f32),
                pltpu.SemaphoreType.DMA((devices, blocks)),
                pltpu.SemaphoreType.DMA(()),
            ],
            name="pack",
        )(sharer_values, queries)
        got = here(exchange(send))
        mean = pl.pallas_call(
            functools.partial(align_kernel, blocks=blocks, slice_len=slice_len),
            out_shape=shape((devices, blocks * slice_len, width), bf16),
            in_specs=[SMEM, SMEM, VMEM],
            out_specs=ANY,
            scratch_shapes=[
                pltpu.VMEM((devices, blocks * slice_len, width), bf16),
                pltpu.VMEM((total, slice_len, width), f32),
                pltpu.SMEM((total,), jnp.int32),
                pltpu.SemaphoreType.DMA((devices,)),
            ],
            name="align",
        )(owner, block_slot, got)
        aligned = exchange(mean)
        asked = got
    else:
        pieces = sharer_values.reshape(blocks, devices, slice_len * width).transpose(1, 0, 2)
        got = exchange(pieces).reshape(total, slice_len * width)
        dest = owner * blocks + block_slot
        hot = (dest[None, :] == jnp.arange(total, dtype=jnp.int32)[:, None]).astype(bf16)
        sums = jnp.dot(hot, got, preferred_element_type=f32)
        count = jnp.sum(hot.astype(f32), axis=1, keepdims=True)
        mean = (sums / jnp.maximum(count, 1.0)).astype(bf16)
        aligned = exchange(mean.reshape(devices, blocks, slice_len * width))
        aligned = aligned.reshape(devices, blocks, slice_len, width).transpose(1, 0, 2, 3)
        aligned = aligned.reshape(tokens, width)
        asked = lax.all_gather(queries.reshape(1, heads * G, DH), "ctx", axis=0, tiled=True)

    weights, part, gate_v, up_v, down_v = pl.pallas_call(
        functools.partial(score_kernel, heads=heads),
        out_shape=(
            shape((heads, rows * G, tokens), bf16),
            shape((rows, heads * G + STAT, DH), f32),
            near(mixer_gate.shape, bf16),
            near(mixer_up.shape, bf16),
            near(mixer_down.shape, bf16),
        ),
        in_specs=[SMEM] + [VMEM] * 4 + [ANY] * 3,
        scratch_shapes=[pltpu.SemaphoreType.DMA((3,))],
        cost_estimate=pl.CostEstimate(
            flops=2 * heads * rows * G * tokens * DH,
            bytes_accessed=2 * 10**6,
            transcendentals=heads * rows * G * tokens,
        ),
        name="score",
    )(
        place, asked, recv_keys, new_keys, new_values, mixer_gate, mixer_up, mixer_down
    )
    merged, numer = pl.pallas_call(
        functools.partial(mixer_kernel, blocks=blocks, slice_len=slice_len if tiled else 0),
        out_shape=(shape((tokens, width), bf16), near(part.shape, f32)),
        in_specs=[SMEM] + [VMEM] * 7,
        name="mixer",
    )(
        gate_logit, here(aligned), recv_values, here(gate_v), here(up_v), here(down_v),
        weights, part,
    )
    attended = pl.pallas_call(
        functools.partial(combine_kernel, heads=heads),
        out_shape=shape((1, heads * G * DH), bf16),
        scratch_shapes=[pltpu.VMEM((heads * G, DH), f32)],
        name="combine",
    )(here(exchange(numer)))
    return merged, attended


def solution(mesh):
    rows = P(("grp", "ctx"), "head")
    return jax.shard_map(
        body,
        mesh=mesh,
        in_specs=(P("grp", None), P("grp"), rows, rows, rows, rows, rows, rows, P(), P(), P(), P("head")),
        out_specs=(rows, rows),
        check_vma=False,
    )
```

```python
import functools
import math

import jax
import jax.numpy as jnp
from jax import lax
from jax.experimental import pallas as pl
from jax.experimental.pallas import tpu as pltpu
from jax.sharding import PartitionSpec as P

DH = 128
BLK = 128
G = 8
STAT = 8
NEG = -1e30
SMEM = pl.BlockSpec(memory_space=pltpu.SMEM)
VMEM = pl.BlockSpec(memory_space=pltpu.VMEM)
ANY = pl.BlockSpec(memory_space=pl.ANY)


def exchange(x):
    return lax.all_to_all(x, "ctx", split_axis=0, concat_axis=0, tiled=True)


def query_tile(query_ref, scratch):
    for r in range(scratch.shape[0]):
        scratch[r : r + 1, :] = query_ref[0:1, r * DH : (r + 1) * DH].astype(jnp.float32)
    return scratch[...].astype(jnp.bfloat16)


def pack_kernel(
    owner_hbm, slot_hbm, sharer_hbm, query_hbm, out_ref, owner_ref, slot_ref, query_ref, scratch, sems, query_sem,
    place_sems, *, blocks, slice_len
):
    devices = out_ref.shape[0]
    copies = [
        pltpu.make_async_copy(owner_hbm, owner_ref, place_sems.at[0]),
        pltpu.make_async_copy(slot_hbm, slot_ref, place_sems.at[1]),
    ]
    for copy in copies:
        copy.start()
    query_copy = pltpu.make_async_copy(query_hbm, query_ref, query_sem)
    query_copy.start()
    width = sharer_hbm.shape[1]
    for d in range(devices):
        for k in range(blocks):
            copies.append(
                pltpu.make_async_copy(
                    sharer_hbm.at[pl.ds(k * BLK + d * slice_len, slice_len), :],
                    out_ref.at[d, pl.ds(k * slice_len, slice_len), pl.ds(0, width)],
                    sems.at[d, k],
                )
            )
            copies[-1].start()
    query_copy.wait()
    q = query_tile(query_ref, scratch)
    for d in range(devices):
        out_ref[d, :, width:] = q
    for copy in copies:
        copy.wait()


def align_kernel(
    owner_ref, slot_ref, got_ref, out_hbm, out_ref, sums, counts, sems, *, blocks, slice_len
):
    devices = out_ref.shape[0]
    width = out_ref.shape[2]
    total = devices * blocks
    sums[...] = jnp.zeros(sums.shape, jnp.float32)
    for r in range(total):
        counts[r] = 0
    for b in range(total):
        dest = owner_ref[b] * blocks + slot_ref[b]
        s, k = divmod(b, blocks)
        sums[dest] += got_ref[s, k * slice_len : (k + 1) * slice_len, :width].astype(jnp.float32)
        counts[dest] = counts[dest] + 1
    copies = []
    for r in range(total):
        d, k = divmod(r, blocks)
        many = jnp.full((1, width), jnp.maximum(counts[r], 1), jnp.int32).astype(jnp.float32)
        out_ref[d, k * slice_len : (k + 1) * slice_len, :] = (sums[r] / many).astype(jnp.bfloat16)
        if k == blocks - 1:
            copies.append(pltpu.make_async_copy(out_ref.at[d], out_hbm.at[d], sems.at[d]))
            copies[-1].start()
    for copy in copies:
        copy.wait()


def score_kernel(
    place_ref, got_ref, key_ref, new_key_ref, new_value_ref, gate_hbm, up_hbm, down_hbm,
    weight_ref, part_ref, gate_ref, up_ref, down_ref, sems, *, heads
):
    pairs = ((gate_hbm, gate_ref), (up_hbm, up_ref), (down_hbm, down_ref))
    copies = [pltpu.make_async_copy(a, b, sems.at[i]) for i, (a, b) in enumerate(pairs)]
    for copy in copies:
        copy.start()
    rows = got_ref.shape[0]
    scale = 1.0 / math.sqrt(DH)
    q_all = got_ref[:, :, got_ref.shape[2] - DH :].astype(jnp.float32)
    row_of = lax.broadcasted_iota(jnp.int32, (rows * G, 1), 0) // G
    allowed = row_of >= place_ref[0]
    sub = lax.broadcasted_iota(jnp.int32, (1, G, DH), 1)
    lane = lax.broadcasted_iota(jnp.int32, (1, G, DH), 2)
    tops = jnp.zeros((rows, 1, DH), jnp.float32)
    dens = jnp.zeros((rows, 1, DH), jnp.float32)
    for j in range(heads):
        cols = slice(j * DH, (j + 1) * DH)
        q = q_all[:, j * G : (j + 1) * G, :].reshape(rows * G, DH)
        s = (
            lax.dot_general(
                q.astype(jnp.bfloat16),
                key_ref[:, cols],
                (((1,), (1,)), ((), ())),
                preferred_element_type=jnp.float32,
            )
            * scale
        )
        sf = jnp.sum(q * new_key_ref[0:1, cols].astype(jnp.float32), axis=1, keepdims=True) * scale
        top = jnp.maximum(
            jnp.max(s, axis=1, keepdims=True), jnp.where(allowed, sf, NEG)
        )
        w = jnp.exp(s - top)
        wf = jnp.where(allowed, jnp.exp(jnp.where(allowed, sf, top) - top), 0.0)
        den = jnp.sum(w, axis=1, keepdims=True) + wf
        weight_ref[j] = w.astype(jnp.bfloat16)
        fresh = wf.astype(jnp.bfloat16).astype(jnp.float32) * new_value_ref[0:1, cols].astype(
            jnp.float32
        )
        part_ref[:, j * G : (j + 1) * G, :] = fresh.reshape(rows, G, DH)
        here = lane == sub + j * G
        spread = lambda v: jnp.sum(
            jnp.where(here, jnp.broadcast_to(v, (rows * G, DH)).reshape(rows, G, DH), 0.0),
            axis=1,
            keepdims=True,
        )
        tops += spread(top)
        dens += spread(den)
    part_ref[:, heads * G :, :] = jnp.where(
        sub == 0, jnp.broadcast_to(tops, (rows, STAT, DH)), jnp.broadcast_to(dens, (rows, STAT, DH))
    )
    for copy in copies:
        copy.wait()
    gate_ref[...] = gate_ref[...] * 0.5


def mixer_kernel(
    logit_ref, got_ref, value_ref, gate_ref, up_ref, down_ref, weight_ref, part_ref, merged_ref, out_ref,
    *, blocks, slice_len
):
    heads = value_ref.shape[1] // DH
    rows = part_ref.shape[0]
    out_ref[:, heads * G :, :] = part_ref[:, heads * G :, :]
    updates = []
    for j in range(heads):
        cols = slice(j * DH, (j + 1) * DH)
        if slice_len:
            a = jnp.concatenate(
                [
                    got_ref[s, k * slice_len : (k + 1) * slice_len, cols]
                    for k in range(blocks)
                    for s in range(got_ref.shape[0])
                ],
                axis=0,
            )
        else:
            a = got_ref[:, cols]
        x = jnp.concatenate([value_ref[:, cols], a], axis=1)
        half = jnp.dot(x, gate_ref[...], preferred_element_type=jnp.float32)
        u = jnp.dot(x, up_ref[...], preferred_element_type=jnp.float32)
        h = ((half + half * jnp.tanh(half)) * u).astype(jnp.bfloat16)
        updates.append(jnp.dot(h, down_ref[...], preferred_element_type=jnp.float32))
    for j in range(heads):
        cols = slice(j * DH, (j + 1) * DH)
        head_gate = jax.nn.sigmoid(jnp.full((1, DH), logit_ref[j], jnp.float32))
        merged = (value_ref[:, cols].astype(jnp.float32) + head_gate * updates[j]).astype(jnp.bfloat16)
        merged_ref[:, cols] = merged
        numer = jnp.dot(weight_ref[j], merged, preferred_element_type=jnp.float32)
        out_ref[:, j * G : (j + 1) * G, :] = part_ref[:, j * G : (j + 1) * G, :] + numer.reshape(
            rows, G, DH
        )


def combine_kernel(got_ref, out_ref, scratch, *, heads):
    n = heads * G
    tops = got_ref[:, n : n + 1, :]
    dens = got_ref[:, n + 1 : n + 2, :]
    factor = jnp.exp(tops - jnp.max(tops, axis=0, keepdims=True))
    factor = factor / jnp.sum(factor * dens, axis=0, keepdims=True)
    sub = lax.broadcasted_iota(jnp.int32, (1, n, DH), 1)
    lane = lax.broadcasted_iota(jnp.int32, (1, n, DH), 2)
    column = jnp.sum(jnp.where(lane == sub, factor, 0.0), axis=2, keepdims=True)
    scratch[...] = jnp.sum(column * got_ref[:, :n, :], axis=0)
    for r in range(n):
        out_ref[0:1, r * DH : (r + 1) * DH] = scratch[r : r + 1, :].astype(jnp.bfloat16)


def body(
    block_owner, block_slot, recv_keys, recv_values, sharer_values, queries, new_keys, new_values,
    mixer_gate, mixer_up, mixer_down, gate_logit,
):
    devices = lax.axis_size("ctx")
    place = lax.axis_index("ctx").astype(jnp.int32).reshape(1)
    tokens, width = recv_values.shape
    heads = width // DH
    blocks = tokens // BLK
    total = blocks * devices
    slice_len = BLK // devices
    owner = block_owner[:, 0]
    rows = devices
    tiled = slice_len % 16 == 0
    f32, bf16 = jnp.float32, jnp.bfloat16
    shape = jax.ShapeDtypeStruct
    near = pltpu.VMEM if tiled else shape

    def here(x):
        return pltpu.with_memory_space_constraint(x, pltpu.VMEM) if tiled else x

    if tiled:
        send, owner_s, slot_s = pl.pallas_call(
            functools.partial(pack_kernel, blocks=blocks, slice_len=slice_len),
            out_shape=(
                near((devices, blocks * slice_len, width + DH), bf16),
                pltpu.SMEM((total,), jnp.int32),
                pltpu.SMEM((total,), jnp.int32),
            ),
            in_specs=[ANY] * 4,
            out_specs=(VMEM, SMEM, SMEM),
            scratch_shapes=[
                pltpu.VMEM(queries.shape, bf16),
                pltpu.VMEM((heads * G, DH), f32),
                pltpu.SemaphoreType.DMA((devices, blocks)),
                pltpu.SemaphoreType.DMA(()),
                pltpu.SemaphoreType.DMA((2,)),
            ],
            name="pack",
        )(owner, block_slot, sharer_values, queries)
        got = here(exchange(send))
        mean = pl.pallas_call(
            functools.partial(align_kernel, blocks=blocks, slice_len=slice_len),
            out_shape=shape((devices, blocks * slice_len, width), bf16),
            in_specs=[SMEM, SMEM, VMEM],
            out_specs=ANY,
            scratch_shapes=[
                pltpu.VMEM((devices, blocks * slice_len, width), bf16),
                pltpu.VMEM((total, slice_len, width), f32),
                pltpu.SMEM((total,), jnp.int32),
                pltpu.SemaphoreType.DMA((devices,)),
            ],
            name="align",
        )(
            pltpu.with_memory_space_constraint(owner_s, pltpu.SMEM),
            pltpu.with_memory_space_constraint(slot_s, pltpu.SMEM),
            got,
        )
        aligned = exchange(mean)
        asked = got
    else:
        pieces = sharer_values.reshape(blocks, devices, slice_len * width).transpose(1, 0, 2)
        got = exchange(pieces).reshape(total, slice_len * width)
        dest = owner * blocks + block_slot
        hot = (dest[None, :] == jnp.arange(total, dtype=jnp.int32)[:, None]).astype(bf16)
        sums = jnp.dot(hot, got, preferred_element_type=f32)
        count = jnp.sum(hot.astype(f32), axis=1, keepdims=True)
        mean = (sums / jnp.maximum(count, 1.0)).astype(bf16)
        aligned = exchange(mean.reshape(devices, blocks, slice_len * width))
        aligned = aligned.reshape(devices, blocks, slice_len, width).transpose(1, 0, 2, 3)
        aligned = aligned.reshape(tokens, width)
        asked = lax.all_gather(queries.reshape(1, heads * G, DH), "ctx", axis=0, tiled=True)

    weights, part, gate_v, up_v, down_v = pl.pallas_call(
        functools.partial(score_kernel, heads=heads),
        out_shape=(
            shape((heads, rows * G, tokens), bf16),
            shape((rows, heads * G + STAT, DH), f32),
            near(mixer_gate.shape, bf16),
            near(mixer_up.shape, bf16),
            near(mixer_down.shape, bf16),
        ),
        in_specs=[SMEM] + [VMEM] * 4 + [ANY] * 3,
        scratch_shapes=[pltpu.SemaphoreType.DMA((3,))],
        cost_estimate=pl.CostEstimate(
            flops=2 * heads * rows * G * tokens * DH,
            bytes_accessed=2 * 10**6,
            transcendentals=heads * rows * G * tokens,
        ),
        name="score",
    )(
        place, asked, recv_keys, new_keys, new_values, mixer_gate, mixer_up, mixer_down
    )
    merged, numer = pl.pallas_call(
        functools.partial(mixer_kernel, blocks=blocks, slice_len=slice_len if tiled else 0),
        out_shape=(shape((tokens, width), bf16), near(part.shape, f32)),
        in_specs=[SMEM] + [VMEM] * 7,
        name="mixer",
    )(
        gate_logit, here(aligned), recv_values, here(gate_v), here(up_v), here(down_v),
        weights, part,
    )
    attended = pl.pallas_call(
        functools.partial(combine_kernel, heads=heads),
        out_shape=shape((1, heads * G * DH), bf16),
        scratch_shapes=[pltpu.VMEM((heads * G, DH), f32)],
        name="combine",
    )(here(exchange(numer)))
    return merged, attended


def solution(mesh):
    rows = P(("grp", "ctx"), "head")
    return jax.shard_map(
        body,
        mesh=mesh,
        in_specs=(P("grp", None), P("grp"), rows, rows, rows, rows, rows, rows, P(), P(), P(), P("head")),
        out_specs=(rows, rows),
        check_vma=False,
    )
```

```python
import functools
import math

import jax
import jax.numpy as jnp
from jax import lax
from jax.experimental import pallas as pl
from jax.experimental.pallas import tpu as pltpu
from jax.sharding import PartitionSpec as P

DH = 128
BLK = 128
G = 8
STAT = 8
NEG = -1e30
SMEM = pl.BlockSpec(memory_space=pltpu.SMEM)
VMEM = pl.BlockSpec(memory_space=pltpu.VMEM)
ANY = pl.BlockSpec(memory_space=pl.ANY)


def exchange(x):
    return lax.all_to_all(x, "ctx", split_axis=0, concat_axis=0, tiled=True)


def query_tile(query_ref, scratch):
    for r in range(scratch.shape[0]):
        scratch[r : r + 1, :] = query_ref[0:1, r * DH : (r + 1) * DH].astype(jnp.float32)
    return scratch[...].astype(jnp.bfloat16)


def pack_kernel(
    owner_hbm, slot_hbm, sharer_hbm, query_hbm, out_ref, owner_ref, slot_ref, query_ref, scratch, sems, query_sem,
    place_sems, *, blocks, slice_len
):
    devices = out_ref.shape[0]
    copies = [
        pltpu.make_async_copy(owner_hbm, owner_ref, place_sems.at[0]),
        pltpu.make_async_copy(slot_hbm, slot_ref, place_sems.at[1]),
    ]
    for copy in copies:
        copy.start()
    query_copy = pltpu.make_async_copy(query_hbm, query_ref, query_sem)
    query_copy.start()
    width = sharer_hbm.shape[1]
    for d in range(devices):
        for k in range(blocks):
            copies.append(
                pltpu.make_async_copy(
                    sharer_hbm.at[pl.ds(k * BLK + d * slice_len, slice_len), :],
                    out_ref.at[d, pl.ds(k * slice_len, slice_len), pl.ds(0, width)],
                    sems.at[d, k],
                )
            )
            copies[-1].start()
    query_copy.wait()
    q = query_tile(query_ref, scratch)
    for d in range(devices):
        out_ref[d, :, width:] = q
    for copy in copies:
        copy.wait()


def align_kernel(
    owner_ref, slot_ref, got_ref, out_hbm, out_ref, sums, counts, sems, *, blocks, slice_len
):
    devices = out_ref.shape[0]
    width = out_ref.shape[2]
    total = devices * blocks
    sums[...] = jnp.zeros(sums.shape, jnp.float32)
    for r in range(total):
        counts[r] = 0
    for b in range(total):
        dest = owner_ref[b] * blocks + slot_ref[b]
        s, k = divmod(b, blocks)
        sums[dest] += got_ref[s, k * slice_len : (k + 1) * slice_len, :width].astype(jnp.float32)
        counts[dest] = counts[dest] + 1
    copies = []
    for r in range(total):
        d, k = divmod(r, blocks)
        many = jnp.full((1, width), jnp.maximum(counts[r], 1), jnp.int32).astype(jnp.float32)
        out_ref[d, k * slice_len : (k + 1) * slice_len, :] = (sums[r] / many).astype(jnp.bfloat16)
        if k == blocks - 1:
            copies.append(pltpu.make_async_copy(out_ref.at[d], out_hbm.at[d], sems.at[d]))
            copies[-1].start()
    for copy in copies:
        copy.wait()


def score_kernel(
    place_ref, got_ref, key_ref, new_key_ref, new_value_ref, gate_hbm, up_hbm, down_hbm,
    weight_ref, part_ref, gate_ref, up_ref, down_ref, sems, *, heads
):
    pairs = ((gate_hbm, gate_ref), (up_hbm, up_ref), (down_hbm, down_ref))
    copies = [pltpu.make_async_copy(a, b, sems.at[i]) for i, (a, b) in enumerate(pairs)]
    for copy in copies:
        copy.start()
    rows = got_ref.shape[0]
    scale = 1.0 / math.sqrt(DH)
    q_all = got_ref[:, :, got_ref.shape[2] - DH :].astype(jnp.float32)
    row_of = lax.broadcasted_iota(jnp.int32, (rows * G, 1), 0) // G
    allowed = row_of >= place_ref[0]
    sub = lax.broadcasted_iota(jnp.int32, (1, G, DH), 1)
    lane = lax.broadcasted_iota(jnp.int32, (1, G, DH), 2)
    tops = jnp.zeros((rows, 1, DH), jnp.float32)
    dens = jnp.zeros((rows, 1, DH), jnp.float32)
    for j in range(heads):
        cols = slice(j * DH, (j + 1) * DH)
        q = q_all[:, j * G : (j + 1) * G, :].reshape(rows * G, DH)
        s = (
            lax.dot_general(
                q.astype(jnp.bfloat16),
                key_ref[:, cols],
                (((1,), (1,)), ((), ())),
                preferred_element_type=jnp.float32,
            )
            * scale
        )
        sf = jnp.sum(q * new_key_ref[0:1, cols].astype(jnp.float32), axis=1, keepdims=True) * scale
        top = jnp.maximum(
            jnp.max(s, axis=1, keepdims=True), jnp.where(allowed, sf, NEG)
        )
        w = jnp.exp(s - top)
        wf = jnp.where(allowed, jnp.exp(jnp.where(allowed, sf, top) - top), 0.0)
        den = jnp.sum(w, axis=1, keepdims=True) + wf
        weight_ref[j] = w.astype(jnp.bfloat16)
        fresh = wf.astype(jnp.bfloat16).astype(jnp.float32) * new_value_ref[0:1, cols].astype(
            jnp.float32
        )
        part_ref[:, j * G : (j + 1) * G, :] = fresh.reshape(rows, G, DH)
        here = lane == sub + j * G
        spread = lambda v: jnp.sum(
            jnp.where(here, jnp.broadcast_to(v, (rows * G, DH)).reshape(rows, G, DH), 0.0),
            axis=1,
            keepdims=True,
        )
        tops += spread(top)
        dens += spread(den)
    part_ref[:, heads * G :, :] = jnp.where(
        sub == 0, jnp.broadcast_to(tops, (rows, STAT, DH)), jnp.broadcast_to(dens, (rows, STAT, DH))
    )
    for copy in copies:
        copy.wait()
    gate_ref[...] = gate_ref[...] * 0.5


def mixer_kernel(
    logit_ref, got_ref, value_ref, gate_ref, up_ref, down_ref, weight_ref, part_ref, merged_hbm, out_ref,
    merged_ref, sems, *, blocks, slice_len
):
    heads = value_ref.shape[1] // DH
    rows = part_ref.shape[0]
    out_ref[:, heads * G :, :] = part_ref[:, heads * G :, :]
    updates = []
    for j in range(heads):
        cols = slice(j * DH, (j + 1) * DH)
        if slice_len:
            a = jnp.concatenate(
                [
                    got_ref[s, k * slice_len : (k + 1) * slice_len, cols]
                    for k in range(blocks)
                    for s in range(got_ref.shape[0])
                ],
                axis=0,
            )
        else:
            a = got_ref[:, cols]
        x = jnp.concatenate([value_ref[:, cols], a], axis=1)
        half = jnp.dot(x, gate_ref[...], preferred_element_type=jnp.float32)
        u = jnp.dot(x, up_ref[...], preferred_element_type=jnp.float32)
        h = ((half + half * jnp.tanh(half)) * u).astype(jnp.bfloat16)
        updates.append(jnp.dot(h, down_ref[...], preferred_element_type=jnp.float32))
    copies = []
    for j in range(heads):
        cols = slice(j * DH, (j + 1) * DH)
        head_gate = jax.nn.sigmoid(jnp.full((1, DH), logit_ref[j], jnp.float32))
        merged = (value_ref[:, cols].astype(jnp.float32) + head_gate * updates[j]).astype(jnp.bfloat16)
        merged_ref[:, cols] = merged
        head = pl.ds(j * DH, DH)
        copies.append(
            pltpu.make_async_copy(merged_ref.at[:, head], merged_hbm.at[:, head], sems.at[j])
        )
        copies[-1].start()
        numer = jnp.dot(weight_ref[j], merged, preferred_element_type=jnp.float32)
        out_ref[:, j * G : (j + 1) * G, :] = part_ref[:, j * G : (j + 1) * G, :] + numer.reshape(
            rows, G, DH
        )
    for copy in copies:
        copy.wait()


def combine_kernel(got_ref, out_ref, scratch, *, heads):
    n = heads * G
    tops = got_ref[:, n : n + 1, :]
    dens = got_ref[:, n + 1 : n + 2, :]
    factor = jnp.exp(tops - jnp.max(tops, axis=0, keepdims=True))
    factor = factor / jnp.sum(factor * dens, axis=0, keepdims=True)
    sub = lax.broadcasted_iota(jnp.int32, (1, n, DH), 1)
    lane = lax.broadcasted_iota(jnp.int32, (1, n, DH), 2)
    column = jnp.sum(jnp.where(lane == sub, factor, 0.0), axis=2, keepdims=True)
    scratch[...] = jnp.sum(column * got_ref[:, :n, :], axis=0)
    for r in range(n):
        out_ref[0:1, r * DH : (r + 1) * DH] = scratch[r : r + 1, :].astype(jnp.bfloat16)


def body(
    block_owner, block_slot, recv_keys, recv_values, sharer_values, queries, new_keys, new_values,
    mixer_gate, mixer_up, mixer_down, gate_logit,
):
    devices = lax.axis_size("ctx")
    place = lax.axis_index("ctx").astype(jnp.int32).reshape(1)
    tokens, width = recv_values.shape
    heads = width // DH
    blocks = tokens // BLK
    total = blocks * devices
    slice_len = BLK // devices
    owner = block_owner[:, 0]
    rows = devices
    tiled = slice_len % 16 == 0
    f32, bf16 = jnp.float32, jnp.bfloat16
    shape = jax.ShapeDtypeStruct
    near = pltpu.VMEM if tiled else shape

    def here(x):
        return pltpu.with_memory_space_constraint(x, pltpu.VMEM) if tiled else x

    if tiled:
        send, owner_s, slot_s = pl.pallas_call(
            functools.partial(pack_kernel, blocks=blocks, slice_len=slice_len),
            out_shape=(
                near((devices, blocks * slice_len, width + DH), bf16),
                pltpu.SMEM((total,), jnp.int32),
                pltpu.SMEM((total,), jnp.int32),
            ),
            in_specs=[ANY] * 4,
            out_specs=(VMEM, SMEM, SMEM),
            scratch_shapes=[
                pltpu.VMEM(queries.shape, bf16),
                pltpu.VMEM((heads * G, DH), f32),
                pltpu.SemaphoreType.DMA((devices, blocks)),
                pltpu.SemaphoreType.DMA(()),
                pltpu.SemaphoreType.DMA((2,)),
            ],
            name="pack",
        )(owner, block_slot, sharer_values, queries)
        got = here(exchange(send))
        mean = pl.pallas_call(
            functools.partial(align_kernel, blocks=blocks, slice_len=slice_len),
            out_shape=shape((devices, blocks * slice_len, width), bf16),
            in_specs=[SMEM, SMEM, VMEM],
            out_specs=ANY,
            scratch_shapes=[
                pltpu.VMEM((devices, blocks * slice_len, width), bf16),
                pltpu.VMEM((total, slice_len, width), f32),
                pltpu.SMEM((total,), jnp.int32),
                pltpu.SemaphoreType.DMA((devices,)),
            ],
            name="align",
        )(
            pltpu.with_memory_space_constraint(owner_s, pltpu.SMEM),
            pltpu.with_memory_space_constraint(slot_s, pltpu.SMEM),
            got,
        )
        aligned = exchange(mean)
        asked = got
    else:
        pieces = sharer_values.reshape(blocks, devices, slice_len * width).transpose(1, 0, 2)
        got = exchange(pieces).reshape(total, slice_len * width)
        dest = owner * blocks + block_slot
        hot = (dest[None, :] == jnp.arange(total, dtype=jnp.int32)[:, None]).astype(bf16)
        sums = jnp.dot(hot, got, preferred_element_type=f32)
        count = jnp.sum(hot.astype(f32), axis=1, keepdims=True)
        mean = (sums / jnp.maximum(count, 1.0)).astype(bf16)
        aligned = exchange(mean.reshape(devices, blocks, slice_len * width))
        aligned = aligned.reshape(devices, blocks, slice_len, width).transpose(1, 0, 2, 3)
        aligned = aligned.reshape(tokens, width)
        asked = lax.all_gather(queries.reshape(1, heads * G, DH), "ctx", axis=0, tiled=True)

    weights, part, gate_v, up_v, down_v = pl.pallas_call(
        functools.partial(score_kernel, heads=heads),
        out_shape=(
            shape((heads, rows * G, tokens), bf16),
            shape((rows, heads * G + STAT, DH), f32),
            near(mixer_gate.shape, bf16),
            near(mixer_up.shape, bf16),
            near(mixer_down.shape, bf16),
        ),
        in_specs=[SMEM] + [VMEM] * 4 + [ANY] * 3,
        scratch_shapes=[pltpu.SemaphoreType.DMA((3,))],
        cost_estimate=pl.CostEstimate(
            flops=2 * heads * rows * G * tokens * DH,
            bytes_accessed=2 * 10**6,
            transcendentals=heads * rows * G * tokens,
        ),
        name="score",
    )(
        place, asked, recv_keys, new_keys, new_values, mixer_gate, mixer_up, mixer_down
    )
    merged, numer = pl.pallas_call(
        functools.partial(mixer_kernel, blocks=blocks, slice_len=slice_len if tiled else 0),
        out_shape=(shape((tokens, width), bf16), near(part.shape, f32)),
        in_specs=[SMEM] + [VMEM] * 7,
        out_specs=(ANY, VMEM),
        scratch_shapes=[
            pltpu.VMEM((tokens, width), bf16),
            pltpu.SemaphoreType.DMA((heads,)),
        ],
        name="mixer",
    )(
        gate_logit, here(aligned), recv_values, here(gate_v), here(up_v), here(down_v),
        weights, part,
    )
    attended = pl.pallas_call(
        functools.partial(combine_kernel, heads=heads),
        out_shape=shape((1, heads * G * DH), bf16),
        scratch_shapes=[pltpu.VMEM((heads * G, DH), f32)],
        name="combine",
    )(here(exchange(numer)))
    return merged, attended


def solution(mesh):
    rows = P(("grp", "ctx"), "head")
    return jax.shard_map(
        body,
        mesh=mesh,
        in_specs=(P("grp", None), P("grp"), rows, rows, rows, rows, rows, rows, P(), P(), P(), P("head")),
        out_specs=(rows, rows),
        check_vma=False,
    )
```
